32 devices in a mesh: dp: 8 (over z, x), expert: 4 (over y, core).
Axes of the slice: x: 2, y: 2, z: 4, core: 2. Of those that a mesh axis runs over, the one named last changes fastest.
Arguments:
- out_grad: bfloat16 [8192, 1024], P(('dp', 'expert')), may hold values from -6 to 6
- expert_of: int32 [8192, 1], P(('dp', 'expert')), may hold values from 0 to 3; in each aligned block of 256 rows (0 to 255, 256 to 511, ...) at most 128 rows name the same one
- pre_act: bfloat16 [16384, 4096], P(('dp', 'expert')), may hold values from -6 to 6
- down_weight: bfloat16 [4, 4096, 1024], P('expert', 'dp'), may hold values from -0.09375 to 0.09375
Outputs:
- pre_grad: bfloat16 [16384, 4096], P(('dp', 'expert'))
- weight_grad: float32 [4, 4096, 1024], P('expert', 'dp')
The draws below stay inside these ranges and needn't reach their ends.
Inputs may be any that keep to these rules, and one draw needn't show every extreme that they name: `expert_of`: within each aligned block of 256 rows (the rows of one device) no expert is named by more than 128 rows, and in some blocks one expert is named by exactly 128 rows.
All inputs are finite; a program needn't handle non-finite values.
Results may differ from the reference program's by a relative error of at most 0.0026.
Values may be sent and summed in bfloat16 or wider, within the bound.
A program may use at most 128 MiB of HBM per device.

```python
import math
import jax
import jax.numpy as jnp
import numpy as np
from jax import lax

D = 1024
FF = 4096
TOK_DEV = 256
CAP = 128
EXPERTS = 4
TOKENS = 8192
ROWS = 16384
N_DP = 8
N_EXPERT = 4


def raised(array, stream_key, source, target, parts, factor):
    def block_of(dim):
        return (jnp.arange(array.shape[dim]) // (array.shape[dim] // parts)).reshape((-1,) + (1,) * (array.ndim - 1 - dim))

    one_side = jax.random.permutation(stream_key, parts)[block_of(target)]
    far = (block_of(target) + parts // 2) % parts
    return jnp.where((block_of(source) == one_side) | (block_of(source) == far), factor * array, array)


def block_levels(rng, shape, shards, smallest, largest):
    def one(dim, blocks):
        draws = jax.random.uniform(jax.random.fold_in(jax.random.fold_in(rng, 6), dim), (blocks,), jnp.float32, smallest / len(shards), largest / len(shards))
        return jnp.repeat(jnp.exp(draws), shape[dim] // blocks).reshape((-1,) + (1,) * (len(shape) - dim - 1))

    loudness = one(*shards[0])
    for cut in shards[1:]:
        loudness = loudness * one(*cut)
    return loudness


def routed_block(own_key, own, number, rows, count, top, most, skew):
    sequence = jax.random.permutation(own_key, count)
    heavy_load, usual = shares(count, rows * top, most, skew, True), shares(count, rows * top, most, skew, False)
    places = jnp.arange(count)

    def named(tallies, turn):
        used = int((tallies > 0).sum())
        fixed = max(1, used // 4)
        shifted = fixed + (places - fixed + turn * (used - fixed)) % max(1, count - fixed)
        return jnp.zeros((count,), jnp.int32).at[sequence[jnp.where(places < fixed, places, shifted)]].set(jnp.asarray(tallies, jnp.int32))

    tallies = jnp.where(number % 4 == 0, named(heavy_load, number // 4), named(usual, number - number // 4 - 1))
    mixed = jax.random.permutation(jax.random.fold_in(own, 3), count)
    source_of, taker = mixed[0:count // 2 * 2:2], mixed[1:count // 2 * 2:2]
    slack = jnp.minimum(tallies[source_of] - 1, most - tallies[taker]) // 2
    slack = jnp.where((source_of == sequence[0]) | (taker == sequence[0]) | (tallies[taker] == 0), 0, jnp.maximum(slack, 0))
    shifted = jax.random.randint(jax.random.fold_in(own, 4), (count // 2,), 0, 1 << 20) % (slack + 1)
    tallies = tallies.at[source_of].add(-shifted).at[taker].add(shifted)
    labels = jnp.searchsorted(jnp.cumsum(tallies), jnp.arange(rows * top), side="right").astype(jnp.int32)
    grid = labels.reshape(top, rows).T
    grid = grid[jax.random.permutation(jax.random.fold_in(own, 1), rows)]
    turn = jax.random.randint(jax.random.fold_in(own, 2), (rows, 1), 0, top)
    return jnp.take_along_axis(grid, (jnp.arange(top)[None, :] + turn) % top, axis=1)


def shares(count, total, reach, lean, full):
    portions = [(1 << 20) // math.isqrt(rank ** lean) + 1 for rank in range(1, count + 1)]
    largest = reach if full else min(reach, max(-(-total // count), total * portions[0] // sum(portions)))
    least = 1 if total - largest >= count - 1 else 0
    counts, rest = [largest] + [least] * (count - 1), total - largest - least * (count - 1)
    while rest > 0:
        movable = [i for i in range(1, count) if counts[i] < largest] or [i for i in range(1, count) if counts[i] < reach]
        mass, budget = sum([portions[i] for i in movable]), rest
        for i in movable:
            addition = min(reach - counts[i], max(1, budget * portions[i] // mass), rest)
            counts[i] = counts[i] + addition
            rest = rest - addition
    return np.array(counts)


def gaussian(stream_key, shape, deviation, reach, cuts=(), kind=jnp.bfloat16):
    array = deviation * jax.random.normal(stream_key, shape, jnp.float32)
    if cuts:
        array = array * block_levels(stream_key, shape, cuts, -0.22, 0.18)
    return jnp.clip(array, -reach, reach).astype(kind)


def noise_with(stream_key, dims, deviation, limit, pieces, heavy, kind=jnp.bfloat16):
    values = deviation * jax.random.normal(stream_key, dims, jnp.float32)
    if pieces:
        values = values * block_levels(stream_key, dims, pieces, -0.22, 0.18)
    return jnp.clip(raised(values, jax.random.fold_in(stream_key, 3), *heavy), -limit, limit).astype(kind)


def setup_inputs(seed: int = 0) -> dict:
    keys = jax.random.split(jax.random.key(seed), 5)
    out_grad = gaussian(keys[0], (TOKENS, D), 1.0, 6.0, ((0, 32),))
    expert_of_keys = jax.random.split(jax.random.fold_in(keys[1], 1), TOKENS // TOK_DEV)
    expert_of_turns = jax.random.permutation(jax.random.fold_in(keys[1], 3), TOKENS // TOK_DEV)
    expert_of = jax.vmap(lambda own, number: routed_block(jax.random.fold_in(keys[1], 2), own, number, TOK_DEV, EXPERTS, 1, CAP, 0))(expert_of_keys, expert_of_turns).reshape((TOKENS, 1))
    pre_act = noise_with(keys[2], (ROWS, FF), 1.0, 6.0, ((0, 32),), (0, 1, 32, 2.75))
    down_weight = gaussian(keys[3], (EXPERTS, FF, D), FF ** -0.5, 0.09375, ((0, 4), (1, 8)))
    return dict(out_grad=out_grad, expert_of=expert_of, pre_act=pre_act, down_weight=down_weight)


tanh_scale = 0.7978845608028654
cubic_weight = 0.044715

def activate(values):
    argument = tanh_scale * (values + cubic_weight * values * values * values)
    return 0.5 * values * (1.0 + jnp.tanh(argument))

def derivative(values):
    tangent = jnp.tanh(tanh_scale * (values + cubic_weight * values * values * values))
    return 0.5 * (1.0 + tangent) + 0.5 * values * (1.0 - tangent * tangent) * tanh_scale * (1.0 + 3.0 * cubic_weight * values * values)

def reference(out_grad, expert_of, pre_act, down_weight):
    blocks = N_DP * N_EXPERT
    routed = expert_of[:, 0].reshape(blocks, TOK_DEV)
    onehot = (routed[:, :, None] == jnp.arange(EXPERTS, dtype=jnp.int32)[None, None, :]).astype(jnp.int32)
    position = lax.optimization_barrier(jnp.sum((jnp.cumsum(onehot, axis=1) - onehot) * onehot, axis=2))
    block_id = jnp.arange(blocks, dtype=jnp.int32)[:, None]
    replica = block_id // N_EXPERT
    source = block_id % N_EXPERT
    target = ((replica * EXPERTS + routed) * N_EXPERT + source) * CAP + position
    dispatched = jnp.zeros((ROWS, D), jnp.bfloat16).at[target.reshape(-1).astype(jnp.int32)].set(out_grad)
    grads_in = dispatched.reshape(N_DP, EXPERTS, N_EXPERT * CAP, D)
    pre_in = pre_act.reshape(N_DP, EXPERTS, N_EXPERT * CAP, FF)
    weights32 = down_weight.astype(jnp.float32)

    def accumulate(running, inputs):
        arrived, pre_rows = inputs
        pre32 = pre_rows.astype(jnp.float32)
        arrived32 = arrived.astype(jnp.float32)
        hidden_grad = jnp.einsum('erd,efd->erf', arrived32, weights32)
        pre_grad = (hidden_grad * derivative(pre32)).astype(jnp.bfloat16)
        hidden = activate(pre32).astype(jnp.bfloat16)
        partial_value = jnp.einsum('erf,erd->efd', hidden.astype(jnp.float32), arrived32)
        return (running + partial_value, pre_grad)
    running, pre_grads = lax.scan(accumulate, jnp.zeros((EXPERTS, FF, D), jnp.float32), (grads_in, pre_in))
    factor = jnp.float32(1.0 / math.sqrt(N_DP * TOK_DEV))
    return (pre_grads.reshape(ROWS, FF), running * factor)
```

```python
import functools
import math

import jax
import jax.numpy as jnp
from jax import lax
from jax.experimental import pallas as pl
from jax.experimental.pallas import tpu as pltpu
from jax.sharding import PartitionSpec as P

tanh_scale = 0.7978845608028654
cubic_weight = 0.044715
MESH = pl.DeviceIdType.MESH
PAIR = 2
LINE = 4
CUTS = 2


def activate(values):
    argument = tanh_scale * (values + cubic_weight * values * values * values)
    return 0.5 * values * (1.0 + jnp.tanh(argument))


def derivative(values):
    tangent = jnp.tanh(tanh_scale * (values + cubic_weight * values * values * values))
    return 0.5 * (1.0 + tangent) + 0.5 * values * (1.0 - tangent * tangent) * tanh_scale * (
        1.0 + 3.0 * cubic_weight * values * values
    )


def kernel(
    experts,
    capacity,
    factor,
    tokens_hbm,
    route_hbm,
    pre_hbm,
    weight_hbm,
    grad_hbm,
    dw_hbm,
    tokens_ref,
    route_ref,
    their_tokens,
    their_route,
    outgoing,
    arrived,
    pre_own,
    pre_theirs,
    weights,
    hidden,
    slope,
    partial,
    sums_out,
    sums_in,
    input_sems,
    token_sems,
    send_sems,
    arrive_sems,
    local_sems,
    pre_sems,
    weight_send,
    weight_recv,
    sum_send,
    sum_recv,
    grad_sems,
):
    d = lax.axis_index("dp")
    me = lax.axis_index("expert")
    z = lax.div(d, PAIR)
    x = lax.rem(d, PAIR)
    partner = z * PAIR + 1 - x
    rows, width = pre_hbm.shape[0], tokens_ref.shape[1]
    block = weight_hbm.shape[0]
    count = tokens_ref.shape[0]
    low = z < LINE // 2

    def order(i):
        if i == LINE - 1:
            return z
        down = LINE - 1 - i
        return jnp.where(
            low, jnp.where(down > z, down, down - 1), jnp.where(i < z, i, i + 1)
        )

    piece = block // CUTS

    def columns(j, side):
        return pl.ds(pl.multiple_of((j * PAIR + side) * block, block), block)

    def within(cut):
        return pl.ds(pl.multiple_of(cut * piece, piece), piece)

    route_load = pltpu.make_async_copy(route_hbm, route_ref, input_sems.at[0])
    token_load = pltpu.make_async_copy(tokens_hbm, tokens_ref, input_sems.at[1])
    route_load.start()
    token_load.start()

    barrier = pltpu.get_barrier_semaphore()
    pl.semaphore_signal(barrier, inc=1, device_id={"dp": partner}, device_id_type=MESH)
    for k in range(1, experts):
        pl.semaphore_signal(
            barrier, inc=1, device_id={"expert": lax.rem(me + k, experts)}, device_id_type=MESH
        )

    @pl.when(z > 0)
    def _():
        pl.semaphore_signal(barrier, inc=1, device_id={"dp": d - PAIR}, device_id_type=MESH)

    @pl.when(z < LINE - 1)
    def _():
        pl.semaphore_signal(barrier, inc=1, device_id={"dp": d + PAIR}, device_id_type=MESH)

    inner = jnp.where((z > 0) & (z < LINE - 1), 2, 1)
    pl.semaphore_wait(barrier, experts + inner)

    def remote(src, dst, send, recv, device):
        return pltpu.make_async_remote_copy(
            src_ref=src, dst_ref=dst, send_sem=send, recv_sem=recv,
            device_id=device, device_id_type=MESH,
        )

    route_copy = remote(
        route_hbm, their_route, token_sems.at[0], token_sems.at[1], {"dp": partner}
    )
    token_copy = remote(
        tokens_hbm, their_tokens, token_sems.at[2], token_sems.at[3], {"dp": partner}
    )
    route_copy.start()
    token_copy.start()

    def weight_copy(direction, hop):
        step = 1 - 2 * direction
        shard = z - step * hop
        shard = jnp.clip(shard, 0, LINE - 1)
        src = weight_hbm if hop == 0 else weights.at[shard]
        return remote(
            src, weights.at[shard], weight_send.at[direction, hop],
            weight_recv.at[direction, hop], {"dp": d + step * PAIR},
        )

    def sends(direction, hop):
        if direction == 0:
            return (z >= hop) & (z < LINE - 1)
        return (z <= LINE - 1 - hop) & (z > 0)

    def receives(direction, hop):
        return (z > hop) if direction == 0 else (z < LINE - 1 - hop)

    def weight_start(hop):
        for direction in range(2):
            @pl.when(sends(direction, hop))
            def _():
                weight_copy(direction, hop).start()

    def weight_arrive(hop):
        for direction in range(2):
            @pl.when(receives(direction, hop))
            def _():
                step = 1 - 2 * direction
                shard = jnp.clip(z - step * (hop + 1), 0, LINE - 1)
                remote(
                    weight_hbm, weights.at[shard], weight_send.at[direction, hop],
                    weight_recv.at[direction, hop], {"dp": partner},
                ).wait_recv()

    weight_start(0)

    def pre_copy(i, cut):
        start = (order(i) * PAIR + 1 - x) * block + cut * piece
        return remote(
            pre_hbm.at[:, pl.ds(pl.multiple_of(start, piece), piece)],
            pre_theirs.at[i, :, within(cut)],
            pre_sems.at[0, i, cut], pre_sems.at[1, i, cut], {"dp": partner},
        )

    for i in range(LINE):
        for cut in range(CUTS):
            pre_copy(i, cut).start()

    def own_copy(i):
        return pltpu.make_async_copy(
            pre_hbm.at[:, columns(order(i), x)], pre_own.at[i], local_sems.at[i]
        )

    for i in range(LINE):
        own_copy(i).start()
    weight_own = pltpu.make_async_copy(weight_hbm, weights.at[z], local_sems.at[LINE])
    weight_own.start()

    def slots(source):
        return pl.ds(pl.multiple_of(source * capacity, capacity), capacity)

    def arrival(rep, k):
        source = lax.rem(me + experts - k, experts)
        return remote(
            outgoing.at[rep, k - 1],
            arrived.at[rep, slots(source)],
            send_sems.at[rep, k - 1],
            arrive_sems.at[rep, k - 1],
            {"expert": lax.rem(me + k, experts)},
        )

    earlier = (
        lax.broadcasted_iota(jnp.int32, (count, count), 0)
        < lax.broadcasted_iota(jnp.int32, (count, count), 1)
    ).astype(jnp.float32).astype(jnp.bfloat16)

    def dispatch(rep, routes, tokens):
        names = routes[...]
        named = lax.broadcasted_iota(jnp.int32, (8, count), 0) == names
        onehot = named.astype(jnp.float32)
        before = jnp.dot(
            onehot.astype(jnp.bfloat16), earlier, preferred_element_type=jnp.float32
        )
        position = jnp.sum(onehot * before, axis=0, keepdims=True).astype(jnp.int32)
        slot = lax.broadcasted_iota(jnp.int32, (capacity, count), 0)
        for k in list(range(1, experts)) + [0]:
            target = lax.rem(me + k, experts)
            place = jnp.where(names == target, position, -1)
            choose = (slot == place).astype(jnp.float32).astype(jnp.bfloat16)
            rows_out = jnp.dot(
                choose, tokens[...], preferred_element_type=jnp.float32
            ).astype(jnp.bfloat16)
            if k == 0:
                arrived[rep, slots(me), :] = rows_out
            else:
                outgoing[rep, k - 1] = rows_out
                remote(
                    outgoing.at[rep, k - 1],
                    arrived.at[rep, slots(me)],
                    send_sems.at[rep, k - 1],
                    arrive_sems.at[rep, k - 1],
                    {"expert": target},
                ).start()

    route_load.wait()
    token_load.wait()
    dispatch(0, route_ref, tokens_ref)

    strip = 64

    def activate_rows(rep, i, source, cut):
        at_columns = within(cut)

        @pl.loop(0, rows // (2 * strip))
        def _(t):
            for half in range(2):
                at = pl.ds(pl.multiple_of(t * 2 * strip + half * strip, strip), strip)
                v = source[i, at, at_columns].astype(jnp.float32)
                square = v * v
                tangent = jnp.tanh(tanh_scale * v * (1.0 + cubic_weight * square))
                gate = 0.5 * (1.0 + tangent)
                slope[rep, i, at, at_columns] = gate + 0.5 * v * (
                    1.0 - tangent * tangent
                ) * tanh_scale * (1.0 + 3.0 * cubic_weight * square)
                hidden[rep, i, at, at_columns] = (v * gate).astype(jnp.bfloat16)

    route_copy.wait_recv()
    token_copy.wait_recv()
    dispatch(1, their_route, their_tokens)
    for i in range(LINE):
        own_copy(i).wait()

        @pl.loop(0, CUTS)
        def _(cut):
            activate_rows(0, i, pre_own, cut)

    weight_arrive(0)
    weight_start(1)
    for rep in range(2):
        for k in range(1, experts):
            arrival(rep, k).wait_recv()

    tile = 256

    def multiply(i):
        @pl.loop(0, CUTS)
        def _(cut):
            pre_copy(i, cut).wait_recv()
            activate_rows(1, i, pre_theirs, cut)
            at = within(cut)
            total = lax.dot_general(
                hidden[0, i, :, at], arrived[0], (((0,), (0,)), ((), ())),
                preferred_element_type=jnp.float32,
            )
            partial[i, at, :] = total + lax.dot_general(
                hidden[1, i, :, at], arrived[1], (((0,), (0,)), ((), ())),
                preferred_element_type=jnp.float32,
            )
            if i < LINE - 1:
                pass_on(i, True, cut)

    def sum_copy(direction, stage, cut):
        part = within(cut)
        return remote(
            sums_out.at[direction, stage, part], sums_in.at[direction, stage, part],
            sum_send.at[direction, stage, cut], sum_recv.at[direction, stage, cut],
            {"dp": d + (1 - 2 * direction) * PAIR},
        )

    def pass_on(i, ends, cut):
        j = order(i)
        part = within(cut)
        for direction in range(2):
            distance = (j - z) if direction == 0 else (z - j)
            first = (z == 0) if direction == 0 else (z == LINE - 1)
            stage = jnp.clip(LINE - 1 - distance, 0, LINE - 2)
            if ends:
                @pl.when((distance > 0) & first)
                def _():
                    sums_out[direction, stage, part, :] = partial[i, part, :].astype(
                        jnp.bfloat16
                    )
                    sum_copy(direction, stage, cut).start()
            else:
                @pl.when((distance > 0) & jnp.logical_not(first))
                def _():
                    last = jnp.clip(stage - 1, 0, LINE - 2)
                    sum_copy(direction, last, cut).wait_recv()
                    sums_out[direction, stage, part, :] = (
                        partial[i, part, :]
                        + sums_in[direction, last, part, :].astype(jnp.float32)
                    ).astype(jnp.bfloat16)
                    sum_copy(direction, stage, cut).start()

    def forward(*blocks):
        @pl.loop(0, CUTS)
        def _(cut):
            for i in blocks:
                pass_on(i, False, cut)

    def grad_copy(i):
        return remote(
            pre_theirs.at[i], grad_hbm.at[:, columns(order(i), x)],
            grad_sems.at[0, i], grad_sems.at[1, i], {"dp": partner},
        )

    def grad_arrive(i):
        return remote(
            pre_theirs.at[i], grad_hbm.at[:, columns(order(i), 1 - x)],
            grad_sems.at[0, i], grad_sems.at[1, i], {"dp": partner},
        )

    def grad_write(i):
        return pltpu.make_async_copy(
            pre_own.at[i], grad_hbm.at[:, columns(order(i), x)], grad_sems.at[2, i]
        )

    def differentiate(i):
        j = order(i)
        for rep, result in ((1, pre_theirs), (0, pre_own)):
            @pl.loop(0, rows // tile)
            def _(t):
                at = pl.ds(pl.multiple_of(t * tile, tile), tile)
                product = lax.dot_general(
                    arrived[rep, at, :], weights[j], (((1,), (1,)), ((), ())),
                    preferred_element_type=jnp.float32,
                )
                result[i, at, :] = (product * slope[rep, i, at, :]).astype(jnp.bfloat16)

            if rep == 1:
                grad_copy(i).start()
            else:
                grad_write(i).start()

    multiply(0)
    multiply(1)
    weight_arrive(1)
    weight_start(2)
    weight_own.wait()
    forward(0)
    multiply(2)
    differentiate(2)
    differentiate(1)
    multiply(3)
    differentiate(3)
    weight_arrive(2)
    differentiate(0)
    forward(1, 2)

    def result_copy(cut):
        part = pl.ds(cut * piece, piece)
        return pltpu.make_async_copy(
            partial.at[LINE - 1, part], dw_hbm.at[part], local_sems.at[LINE + 1 + cut]
        )

    for cut in range(CUTS):
        part = pl.ds(cut * piece, piece)
        for direction in range(2):
            @pl.when(receives(direction, 0))
            def _():
                sum_copy(direction, LINE - 2, cut).wait_recv()
                partial[LINE - 1, part, :] += sums_in[direction, LINE - 2, part, :].astype(jnp.float32)
        partial[LINE - 1, part, :] = partial[LINE - 1, part, :] * factor
        result_copy(cut).start()

    for i in range(LINE):
        grad_arrive(i).wait_recv()
        grad_write(i).wait()
    for cut in range(CUTS):
        result_copy(cut).wait()
    route_copy.wait_send()
    token_copy.wait_send()
    for i in range(LINE):
        for cut in range(CUTS):
            pre_copy(i, cut).wait_send()
        grad_copy(i).wait_send()
    for rep in range(2):
        for k in range(1, experts):
            arrival(rep, k).wait_send()
    for hop in range(LINE - 1):
        for direction in range(2):
            @pl.when(sends(direction, hop))
            def _():
                weight_copy(direction, hop).wait_send()
    for stage in range(LINE - 1):
        for direction in range(2):
            toward = (z <= stage) if direction == 0 else (z >= LINE - 1 - stage)
            inside = (z < LINE - 1) if direction == 0 else (z > 0)

            @pl.when(toward & inside)
            def _():
                for cut in range(CUTS):
                    sum_copy(direction, stage, cut).wait_send()


def fused(out_grad, expert_of, pre_act, down_weight):
    experts = lax.axis_size("expert")
    replicas = lax.axis_size("dp")
    count, width = out_grad.shape
    rows, units = pre_act.shape
    block = down_weight.shape[1]
    capacity = count // 2
    factor = 1.0 / math.sqrt(replicas * count)
    half, full = jnp.bfloat16, jnp.float32
    hbm = pl.BlockSpec(memory_space=pltpu.HBM)
    anywhere = pl.BlockSpec(memory_space=pl.ANY)
    dma = pltpu.SemaphoreType.DMA
    pre_grad, summed = pl.pallas_call(
        functools.partial(kernel, experts, capacity, factor),
        out_shape=(
            jax.ShapeDtypeStruct((rows, units), half),
            jax.ShapeDtypeStruct((block, width), full),
        ),
        in_specs=[hbm, hbm, hbm, hbm],
        out_specs=(anywhere, anywhere),
        scratch_shapes=[
            pltpu.VMEM((count, width), half),
            pltpu.VMEM((1, count), jnp.int32),
            pltpu.VMEM((count, width), half),
            pltpu.VMEM((1, count), jnp.int32),
            pltpu.VMEM((2, experts - 1, capacity, width), half),
            pltpu.VMEM((2, rows, width), half),
            pltpu.VMEM((LINE, rows, block), half),
            pltpu.VMEM((LINE, rows, block), half),
            pltpu.VMEM((LINE, block, width), half),
            pltpu.VMEM((2, LINE, rows, block), half),
            pltpu.VMEM((2, LINE, rows, block), full),
            pltpu.VMEM((LINE, block, width), full),
            pltpu.VMEM((2, LINE - 1, block, width), half),
            pltpu.VMEM((2, LINE - 1, block, width), half),
            dma((2,)),
            dma((4,)),
            dma((2, experts - 1)),
            dma((2, experts - 1)),
            dma((LINE + 1 + CUTS,)),
            dma((2, LINE, CUTS)),
            dma((2, LINE - 1)),
            dma((2, LINE - 1)),
            dma((2, LINE - 1, CUTS)),
            dma((2, LINE - 1, CUTS)),
            dma((3, LINE)),
        ],
        compiler_params=pltpu.CompilerParams(
            collective_id=0, has_side_effects=True, vmem_limit_bytes=46 * 1024 * 1024
        ),
    )(*(
        pltpu.with_memory_space_constraint(array, pltpu.HBM)
        for array in (out_grad, expert_of.reshape(1, count), pre_act, down_weight[0])
    ))
    return pre_grad, summed.reshape(1, block, width)


def body(out_grad, expert_of, pre_act, down_weight):
    experts = lax.axis_size("expert")
    replicas = lax.axis_size("dp")
    if replicas == PAIR * LINE and experts <= 8:
        return fused(out_grad, expert_of, pre_act, down_weight)
    token_count = out_grad.shape[0]
    model_width = out_grad.shape[1]
    capacity = token_count // 2
    routed = expert_of[:, 0]
    onehot = (routed[:, None] == jnp.arange(experts, dtype=jnp.int32)[None, :]).astype(jnp.int32)
    position = jnp.sum((jnp.cumsum(onehot, axis=0) - onehot) * onehot, axis=1)
    target = routed * capacity + position
    outgoing = jnp.zeros((experts * capacity, model_width), jnp.bfloat16).at[target].set(out_grad)
    arrived = lax.all_to_all(
        outgoing.reshape(experts, capacity, model_width),
        "expert",
        split_axis=0,
        concat_axis=0,
        tiled=True,
    )
    arrived = arrived.reshape(experts * capacity, model_width)
    weight = down_weight[0]
    own_rows = weight.shape[0]
    factor = 1.0 / math.sqrt(replicas * token_count)
    hidden_grad = lax.dot_general(
        arrived,
        lax.all_gather(weight, "dp", axis=0, tiled=True),
        (((1,), (1,)), ((), ())),
        preferred_element_type=jnp.float32,
    )
    pre_block = pre_act.astype(jnp.float32)
    pre_grad = (hidden_grad * derivative(pre_block)).astype(jnp.bfloat16)
    hidden = activate(pre_block).astype(jnp.bfloat16)
    summed = lax.psum_scatter(
        lax.dot_general(
            hidden, arrived, (((0,), (0,)), ((), ())), preferred_element_type=jnp.float32
        ),
        "dp",
        scatter_dimension=0,
        tiled=True,
    )
    return (pre_grad, (summed * factor).reshape(1, own_rows, model_width))


def solution(mesh):
    placed = (
        P(("dp", "expert"), None),
        P(("dp", "expert"), None),
        P(("dp", "expert"), None),
        P("expert", "dp", None),
    )
    return jax.shard_map(
        body,
        mesh=mesh,
        in_specs=placed,
        out_specs=(P(("dp", "expert"), None), P("expert", "dp", None)),
        check_vma=False,
    )
```

```python
import functools
import math

import jax
import jax.numpy as jnp
from jax import lax
from jax.experimental import pallas as pl
from jax.experimental.pallas import tpu as pltpu
from jax.sharding import PartitionSpec as P

tanh_scale = 0.7978845608028654
cubic_weight = 0.044715
MESH = pl.DeviceIdType.MESH
PAIR = 2
LINE = 4
CUTS = 2
HALVES = 2
PARTS = 4


def activate(values):
    argument = tanh_scale * (values + cubic_weight * values * values * values)
    return 0.5 * values * (1.0 + jnp.tanh(argument))


def derivative(values):
    tangent = jnp.tanh(tanh_scale * (values + cubic_weight * values * values * values))
    return 0.5 * (1.0 + tangent) + 0.5 * values * (1.0 - tangent * tangent) * tanh_scale * (
        1.0 + 3.0 * cubic_weight * values * values
    )


def kernel(
    experts,
    capacity,
    factor,
    tokens_hbm,
    route_hbm,
    pre_hbm,
    weight_hbm,
    grad_hbm,
    dw_hbm,
    own_tokens,
    own_route,
    their_tokens,
    their_route,
    choose,
    outgoing,
    arrived,
    pre_own,
    pre_theirs,
    lane_in,
    lane_pack,
    lane_got,
    lane_out,
    weights,
    hidden,
    slope,
    partial,
    sums_out,
    sums_in,
    input_sems,
    token_sems,
    dispatch_send,
    dispatch_recv,
    local_sems,
    pre_sems,
    lane_send,
    lane_recv,
    cross_sems,
    weight_send,
    weight_recv,
    sum_send,
    sum_recv,
    grad_sems,
):
    d = lax.axis_index("dp")
    me = lax.axis_index("expert")
    z = lax.div(d, PAIR)
    x = lax.rem(d, PAIR)
    partner = z * PAIR + 1 - x
    rows, width = pre_hbm.shape[0], own_tokens.shape[1]
    block = weight_hbm.shape[0]
    count = own_tokens.shape[0]
    low = z < LINE // 2
    own = LINE - 1
    piece, part_rows, span = block // CUTS, block // PARTS, width // HALVES
    chunks = [(cut, half) for half in range(HALVES) for cut in range(CUTS)]

    def order(i):
        if i == own:
            return z
        down = LINE - 1 - i
        return jnp.where(
            low, jnp.where(down > z, down, down - 1), jnp.where(i < z, i, i + 1)
        )

    def columns(j, side):
        return pl.ds(pl.multiple_of((j * PAIR + side) * block, block), block)

    def within(cut):
        return pl.ds(cut * piece, piece)

    def across(half):
        return pl.ds(half * span, span)

    def slots(source):
        return pl.ds(pl.multiple_of(source * capacity, capacity), capacity)

    def peer(k):
        return lax.rem(me + k, experts)

    def from_peer(k):
        return lax.rem(me + experts - k, experts)

    route_load = pltpu.make_async_copy(route_hbm, own_route, input_sems.at[0])
    token_load = pltpu.make_async_copy(tokens_hbm, own_tokens, input_sems.at[1])
    route_load.start()
    token_load.start()

    barrier = pltpu.get_barrier_semaphore()
    pl.semaphore_signal(barrier, inc=1, device_id={"dp": partner}, device_id_type=MESH)
    for k in range(1, experts):
        pl.semaphore_signal(
            barrier, inc=1, device_id={"expert": peer(k)}, device_id_type=MESH
        )

    @pl.when(z > 0)
    def _():
        pl.semaphore_signal(barrier, inc=1, device_id={"dp": d - PAIR}, device_id_type=MESH)

    @pl.when(z < LINE - 1)
    def _():
        pl.semaphore_signal(barrier, inc=1, device_id={"dp": d + PAIR}, device_id_type=MESH)

    inner = jnp.where((z > 0) & (z < LINE - 1), 2, 1)
    pl.semaphore_wait(barrier, experts + inner)

    def remote(src, dst, send, recv, device):
        return pltpu.make_async_remote_copy(
            src_ref=src, dst_ref=dst, send_sem=send, recv_sem=recv,
            device_id=device, device_id_type=MESH,
        )

    route_copy = remote(
        route_hbm, their_route, token_sems.at[0, HALVES], token_sems.at[1, HALVES],
        {"dp": partner},
    )

    def token_copy(half):
        return remote(
            tokens_hbm.at[:, across(half)], their_tokens.at[:, across(half)],
            token_sems.at[0, half], token_sems.at[1, half], {"dp": partner},
        )

    def pre_copy(i, cut):
        start = (order(i) * PAIR + 1 - x) * block + cut * piece
        return remote(
            pre_hbm.at[:, pl.ds(pl.multiple_of(start, piece), piece)],
            pre_theirs.at[i, :, within(cut)],
            pre_sems.at[0, i, cut], pre_sems.at[1, i, cut], {"dp": partner},
        )

    def cross(lane):
        return remote(
            lane_pack.at[lane], lane_got.at[lane],
            cross_sems.at[0, lane], cross_sems.at[1, lane], {"dp": partner},
        )

    def part(c):
        return pl.ds(c * part_rows, part_rows)

    def weight_copy(direction, hop, c):
        step = 1 - 2 * direction
        shard = jnp.clip(z - step * hop, 0, LINE - 1)
        src = weight_hbm if hop == 0 else weights.at[shard]
        return remote(
            src.at[part(c)], weights.at[shard, part(c)], weight_send.at[direction, hop, c],
            weight_recv.at[direction, hop, c], {"dp": d + step * PAIR},
        )

    def sends(direction, hop):
        if direction == 0:
            return (z >= hop) & (z < LINE - 1)
        return (z <= LINE - 1 - hop) & (z > 0)

    def receives(direction, hop):
        return (z > hop) if direction == 0 else (z < LINE - 1 - hop)

    def weight_start(hop, c):
        for direction in range(2):
            @pl.when(sends(direction, hop))
            def _():
                weight_copy(direction, hop, c).start()

    def weight_arrive(hop, c):
        for direction in range(2):
            @pl.when(receives(direction, hop))
            def _():
                step = 1 - 2 * direction
                shard = jnp.clip(z - step * (hop + 1), 0, LINE - 1)
                remote(
                    weight_hbm.at[part(c)], weights.at[shard, part(c)],
                    weight_send.at[direction, hop, c],
                    weight_recv.at[direction, hop, c], {"dp": partner},
                ).wait_recv()

        if hop < LINE - 2:
            weight_start(hop + 1, c)

    route_copy.start()
    for half in range(HALVES):
        token_copy(half).start()
    for c in range(PARTS):
        weight_start(0, c)
    for i in range(own - 1):
        for cut in range(CUTS):
            pre_copy(i, cut).start()

    def own_copy(i):
        return pltpu.make_async_copy(
            pre_hbm.at[:, columns(order(i), x)], pre_own.at[i], local_sems.at[i]
        )

    for i in range(LINE):
        own_copy(i).start()
    weight_own = pltpu.make_async_copy(weight_hbm, weights.at[z], local_sems.at[LINE])
    weight_own.start()

    earlier = (
        lax.broadcasted_iota(jnp.int32, (count, count), 0)
        < lax.broadcasted_iota(jnp.int32, (count, count), 1)
    ).astype(jnp.float32).astype(jnp.bfloat16)

    def plan(rep, routes):
        names = routes[...]
        named = lax.broadcasted_iota(jnp.int32, (8, count), 0) == names
        onehot = named.astype(jnp.float32)
        before = jnp.dot(
            onehot.astype(jnp.bfloat16), earlier, preferred_element_type=jnp.float32
        )
        position = jnp.sum(onehot * before, axis=0, keepdims=True).astype(jnp.int32)
        slot = lax.broadcasted_iota(jnp.int32, (capacity, count), 0)
        for e in range(experts):
            place = jnp.where(names == e, position, -1)
            choose[rep, e * capacity:(e + 1) * capacity, :] = (
                (slot == place).astype(jnp.float32).astype(jnp.bfloat16)
            )

    def dispatch_copy(rep, k, half):
        return remote(
            outgoing.at[rep, k - 1, :, across(half)],
            arrived.at[rep, slots(me), across(half)],
            dispatch_send.at[rep, k - 1, half],
            dispatch_recv.at[rep, k - 1, half],
            {"expert": peer(k)},
        )

    def dispatch(rep, tokens, half):
        for k in list(range(1, experts)) + [0]:
            rows_out = jnp.dot(
                choose[rep, slots(peer(k)), :], tokens[:, across(half)],
                preferred_element_type=jnp.float32,
            ).astype(jnp.bfloat16)
            if k == 0:
                arrived[rep, slots(me), across(half)] = rows_out
            else:
                outgoing[rep, k - 1, :, across(half)] = rows_out
                dispatch_copy(rep, k, half).start()

    def tokens_arrive(rep, half):
        for k in range(1, experts):
            remote(
                outgoing.at[rep, k - 1, :, across(half)],
                arrived.at[rep, slots(from_peer(k)), across(half)],
                dispatch_send.at[rep, k - 1, half],
                dispatch_recv.at[rep, k - 1, half],
                {"expert": peer(k)},
            ).wait_recv()

    def lane_copy(leg, k):
        target = peer(k)
        if leg == 0:
            src = pre_hbm.at[slots(target), columns(z, 1 - x)]
            dst = lane_in.at[0, slots(me)]
        elif leg == 1:
            src = lane_out.at[0, k - 1]
            dst = pre_theirs.at[own, slots(me)]
        elif leg == 2:
            src = pre_theirs.at[own, slots(target)]
            dst = lane_in.at[1, slots(me)]
        else:
            src = lane_out.at[1, k]
            dst = grad_hbm.at[slots(me), columns(z, 1 - x)]
        return remote(
            src, dst, lane_send.at[leg, k - 1], lane_recv.at[leg, k - 1], {"expert": target}
        )

    def lane_arrive(leg):
        for k in range(1, experts):
            source = from_peer(k)
            if leg == 0:
                dst = lane_in.at[0, slots(source)]
            elif leg == 1:
                dst = pre_theirs.at[own, slots(source)]
            elif leg == 2:
                dst = lane_in.at[1, slots(source)]
            else:
                dst = grad_hbm.at[slots(source), columns(z, 1 - x)]
            remote(
                lane_out.at[0, k - 1], dst, lane_send.at[leg, k - 1], lane_recv.at[leg, k - 1],
                {"expert": peer(k)},
            ).wait_recv()

    lane_local = pltpu.make_async_copy(
        pre_hbm.at[slots(me), columns(z, 1 - x)], lane_in.at[0, slots(me)],
        local_sems.at[LINE + 1],
    )
    lane_home = pltpu.make_async_copy(
        lane_out.at[1, 0], grad_hbm.at[slots(me), columns(z, 1 - x)], local_sems.at[LINE + 2]
    )

    def gather(lane):
        lane_pack[lane] = lax.dot_general(
            choose[lane], lane_in[lane], (((0,), (0,)), ((), ())),
            preferred_element_type=jnp.float32,
        ).astype(jnp.bfloat16)
        cross(lane).start()

    def spread(lane):
        cross(lane).wait_recv()
        for k in list(range(1, experts)) + [0]:
            rows_out = jnp.dot(
                choose[1 - lane, slots(peer(k)), :], lane_got[lane],
                preferred_element_type=jnp.float32,
            ).astype(jnp.bfloat16)
            if lane == 0:
                if k == 0:
                    pre_theirs[own, slots(me), :] = rows_out
                else:
                    lane_out[0, k - 1] = rows_out
                    lane_copy(1, k).start()
            else:
                lane_out[1, k] = rows_out
                if k == 0:
                    lane_home.start()
                else:
                    lane_copy(3, k).start()

    strip = 64

    def activate_rows(rep, i, source, cut):
        at_columns = within(cut)

        @pl.loop(0, rows // (2 * strip))
        def _(t):
            for half in range(2):
                at = pl.ds(pl.multiple_of(t * 2 * strip + half * strip, strip), strip)
                v = source[i, at, at_columns].astype(jnp.float32)
                square = v * v
                tangent = jnp.tanh(tanh_scale * v * (1.0 + cubic_weight * square))
                gate = 0.5 * (1.0 + tangent)
                slope[rep, i, at, at_columns] = gate + 0.5 * v * (
                    1.0 - tangent * tangent
                ) * tanh_scale * (1.0 + 3.0 * cubic_weight * square)
                hidden[rep, i, at, at_columns] = (v * gate).astype(jnp.bfloat16)

    def activate_own(i):
        own_copy(i).wait()
        for cut in range(CUTS):
            activate_rows(0, i, pre_own, cut)

    def activate_theirs(i, cut):
        if i < own:
            pre_copy(i, cut).wait_recv()
        activate_rows(1, i, pre_theirs, cut)

    def term(i, cut, half):
        at, wide = within(cut), across(half)
        total = lax.dot_general(
            hidden[0, i, :, at], arrived[0, :, wide], (((0,), (0,)), ((), ())),
            preferred_element_type=jnp.float32,
        )
        partial[i, at, wide] = total + lax.dot_general(
            hidden[1, i, :, at], arrived[1, :, wide], (((0,), (0,)), ((), ())),
            preferred_element_type=jnp.float32,
        )
        if i < own:
            pass_on(i, True, cut, half)

    def sum_copy(direction, stage, cut, half):
        at, wide = within(cut), across(half)
        return remote(
            sums_out.at[direction, stage, at, wide], sums_in.at[direction, stage, at, wide],
            sum_send.at[direction, stage, cut, half], sum_recv.at[direction, stage, cut, half],
            {"dp": d + (1 - 2 * direction) * PAIR},
        )

    def pass_on(i, ends, cut, half):
        j = order(i)
        at, wide = within(cut), across(half)
        for direction in range(2):
            distance = (j - z) if direction == 0 else (z - j)
            first = (z == 0) if direction == 0 else (z == LINE - 1)
            stage = jnp.clip(LINE - 1 - distance, 0, LINE - 2)
            if ends:
                @pl.when((distance > 0) & first)
                def _():
                    sums_out[direction, stage, at, wide] = partial[i, at, wide].astype(
                        jnp.bfloat16
                    )
                    sum_copy(direction, stage, cut, half).start()
            else:
                @pl.when((distance > 0) & jnp.logical_not(first))
                def _():
                    last = jnp.clip(stage - 1, 0, LINE - 2)
                    sum_copy(direction, last, cut, half).wait_recv()
                    sums_out[direction, stage, at, wide] = (
                        partial[i, at, wide]
                        + sums_in[direction, last, at, wide].astype(jnp.float32)
                    ).astype(jnp.bfloat16)
                    sum_copy(direction, stage, cut, half).start()

    def forward(i, chunk):
        pass_on(i, False, *chunk)

    def grad_copy(i):
        return remote(
            pre_theirs.at[i], grad_hbm.at[:, columns(order(i), x)],
            grad_sems.at[0, i], grad_sems.at[1, i], {"dp": partner},
        )

    def grad_arrive(i):
        return remote(
            pre_theirs.at[i], grad_hbm.at[:, columns(order(i), 1 - x)],
            grad_sems.at[0, i], grad_sems.at[1, i], {"dp": partner},
        )

    def grad_write(i):
        return pltpu.make_async_copy(
            pre_own.at[i], grad_hbm.at[:, columns(order(i), x)], grad_sems.at[2, i]
        )

    tile = 256

    def differentiate(rep, i):
        j = order(i)
        result = pre_theirs if rep == 1 else pre_own

        @pl.loop(0, rows // tile)
        def _(t):
            at = pl.ds(pl.multiple_of(t * tile, tile), tile)
            product = lax.dot_general(
                arrived[rep, at, :], weights[j], (((1,), (1,)), ((), ())),
                preferred_element_type=jnp.float32,
            )
            result[i, at, :] = (product * slope[rep, i, at, :]).astype(jnp.bfloat16)

        if rep == 0:
            grad_write(i).start()
        elif i < own:
            grad_copy(i).start()
        else:
            for k in range(1, experts):
                lane_copy(2, k).start()
            lane_in[1, slots(me), :] = pre_theirs[own, slots(me), :]

    route_load.wait()
    token_load.wait()
    plan(0, own_route)
    dispatch(0, own_tokens, 0)
    activate_own(0)
    activate_own(1)
    route_copy.wait_recv()
    plan(1, their_route)
    token_copy(0).wait_recv()
    dispatch(1, their_tokens, 0)
    dispatch(0, own_tokens, 1)
    activate_own(2)
    weight_arrive(0, 0)
    token_copy(1).wait_recv()
    dispatch(1, their_tokens, 1)
    lane_local.start()
    for k in range(1, experts):
        lane_copy(0, k).start()
    activate_own(own)
    weight_arrive(0, 1)
    for rep in range(2):
        tokens_arrive(rep, 0)
    activate_theirs(0, 0)
    term(0, 0, 0)
    weight_arrive(0, 2)
    activate_theirs(0, 1)
    term(0, 1, 0)
    weight_arrive(0, 3)
    for rep in range(2):
        tokens_arrive(rep, 1)
    term(0, 0, 1)
    term(0, 1, 1)
    weight_own.wait()
    differentiate(0, own)
    differentiate(0, own - 1)
    lane_local.wait()
    lane_arrive(0)
    gather(0)
    for cut in range(CUTS):
        pre_copy(own - 1, cut).start()
    weight_arrive(1, 0)
    forward(0, chunks[0])
    activate_theirs(1, 0)
    weight_arrive(1, 1)
    forward(0, chunks[1])
    activate_theirs(1, 1)
    for chunk in chunks:
        term(1, *chunk)
    weight_arrive(1, 2)
    forward(0, chunks[2])
    spread(0)
    weight_arrive(1, 3)
    forward(0, chunks[3])
    differentiate(1, 1)
    differentiate(0, 1)
    lane_arrive(1)
    for cut in range(CUTS):
        activate_theirs(own, cut)
    differentiate(1, own)
    for cut in range(CUTS):
        activate_theirs(2, cut)
    for chunk in chunks:
        term(2, *chunk)
    differentiate(1, 2)
    forward(1, chunks[0])
    forward(2, chunks[0])
    for chunk in chunks:
        term(own, *chunk)
    lane_arrive(2)
    gather(1)
    for c in range(2):
        weight_arrive(2, c)
    forward(1, chunks[1])
    forward(2, chunks[1])
    forward(1, chunks[2])
    forward(2, chunks[2])
    for c in range(2, PARTS):
        weight_arrive(2, c)
    differentiate(1, 0)
    forward(1, chunks[3])
    forward(2, chunks[3])
    differentiate(0, 0)

    def result_copy(cut, half):
        at, wide = within(cut), across(half)
        return pltpu.make_async_copy(
            partial.at[own, at, wide], dw_hbm.at[at, wide],
            local_sems.at[LINE + 3 + cut * HALVES + half],
        )

    for n, (cut, half) in enumerate(chunks):
        at, wide = within(cut), across(half)
        for direction in range(2):
            @pl.when(receives(direction, 0))
            def _():
                sum_copy(direction, LINE - 2, cut, half).wait_recv()
                partial[own, at, wide] += sums_in[direction, LINE - 2, at, wide].astype(
                    jnp.float32
                )
        partial[own, at, wide] = partial[own, at, wide] * factor
        result_copy(cut, half).start()
        if n == 1:
            spread(1)

    lane_arrive(3)
    lane_home.wait()
    for i in range(LINE):
        if i < own:
            grad_arrive(i).wait_recv()
        grad_write(i).wait()
    for cut, half in chunks:
        result_copy(cut, half).wait()
    route_copy.wait_send()
    for half in range(HALVES):
        token_copy(half).wait_send()
    for i in range(own):
        for cut in range(CUTS):
            pre_copy(i, cut).wait_send()
        grad_copy(i).wait_send()
    for lane in range(2):
        cross(lane).wait_send()
    for k in range(1, experts):
        for leg in range(4):
            lane_copy(leg, k).wait_send()
        for rep in range(2):
            for half in range(HALVES):
                dispatch_copy(rep, k, half).wait_send()
    for hop in range(LINE - 1):
        for direction in range(2):
            @pl.when(sends(direction, hop))
            def _():
                for c in range(PARTS):
                    weight_copy(direction, hop, c).wait_send()
    for stage in range(LINE - 1):
        for direction in range(2):
            toward = (z <= stage) if direction == 0 else (z >= LINE - 1 - stage)
            inside = (z < LINE - 1) if direction == 0 else (z > 0)

            @pl.when(toward & inside)
            def _():
                for cut, half in chunks:
                    sum_copy(direction, stage, cut, half).wait_send()


def fused(out_grad, expert_of, pre_act, down_weight):
    experts = lax.axis_size("expert")
    replicas = lax.axis_size("dp")
    count, width = out_grad.shape
    rows, units = pre_act.shape
    block = down_weight.shape[1]
    capacity = count // 2
    factor = 1.0 / math.sqrt(replicas * count)
    half, full = jnp.bfloat16, jnp.float32
    hbm = pl.BlockSpec(memory_space=pltpu.HBM)
    anywhere = pl.BlockSpec(memory_space=pl.ANY)
    dma = pltpu.SemaphoreType.DMA
    pre_grad, summed = pl.pallas_call(
        functools.partial(kernel, experts, capacity, factor),
        out_shape=(
            pltpu.VMEM((rows, units), half),
            pltpu.VMEM((block, width), full),
        ),
        in_specs=[hbm, hbm, hbm, hbm],
        out_specs=(anywhere, anywhere),
        scratch_shapes=[
            pltpu.VMEM((count, width), half),
            pltpu.VMEM((1, count), jnp.int32),
            pltpu.VMEM((count, width), half),
            pltpu.VMEM((1, count), jnp.int32),
            pltpu.VMEM((2, experts * capacity, count), half),
            pltpu.VMEM((2, experts - 1, capacity, width), half),
            pltpu.VMEM((2, rows, width), half),
            pltpu.VMEM((LINE, rows, block), half),
            pltpu.VMEM((LINE, rows, block), half),
            pltpu.VMEM((2, rows, block), half),
            pltpu.VMEM((2, count, block), half),
            pltpu.VMEM((2, count, block), half),
            pltpu.VMEM((2, experts, capacity, block), half),
            pltpu.VMEM((LINE, block, width), half),
            pltpu.VMEM((2, LINE, rows, block), half),
            pltpu.VMEM((2, LINE, rows, block), full),
            pltpu.VMEM((LINE, block, width), full),
            pltpu.VMEM((2, LINE - 1, block, width), half),
            pltpu.VMEM((2, LINE - 1, block, width), half),
            dma((2,)),
            dma((2, HALVES + 1)),
            dma((2, experts - 1, HALVES)),
            dma((2, experts - 1, HALVES)),
            dma((LINE + 3 + CUTS * HALVES,)),
            dma((2, LINE - 1, CUTS)),
            dma((4, experts - 1)),
            dma((4, experts - 1)),
            dma((2, 2)),
            dma((2, LINE - 1, PARTS)),
            dma((2, LINE - 1, PARTS)),
            dma((2, LINE - 1, CUTS, HALVES)),
            dma((2, LINE - 1, CUTS, HALVES)),
            dma((3, LINE)),
        ],
        compiler_params=pltpu.CompilerParams(
            collective_id=0, has_side_effects=True, vmem_limit_bytes=51 * 1024 * 1024
        ),
    )(*(
        pltpu.with_memory_space_constraint(array, pltpu.HBM)
        for array in (out_grad, expert_of.reshape(1, count), pre_act, down_weight[0])
    ))
    return pre_grad, summed.reshape(1, block, width)


def body(out_grad, expert_of, pre_act, down_weight):
    experts = lax.axis_size("expert")
    replicas = lax.axis_size("dp")
    if replicas == PAIR * LINE and experts <= 8:
        return fused(out_grad, expert_of, pre_act, down_weight)
    token_count = out_grad.shape[0]
    model_width = out_grad.shape[1]
    capacity = token_count // 2
    routed = expert_of[:, 0]
    onehot = (routed[:, None] == jnp.arange(experts, dtype=jnp.int32)[None, :]).astype(jnp.int32)
    position = jnp.sum((jnp.cumsum(onehot, axis=0) - onehot) * onehot, axis=1)
    target = routed * capacity + position
    outgoing = jnp.zeros((experts * capacity, model_width), jnp.bfloat16).at[target].set(out_grad)
    arrived = lax.all_to_all(
        outgoing.reshape(experts, capacity, model_width),
        "expert",
        split_axis=0,
        concat_axis=0,
        tiled=True,
    )
    arrived = arrived.reshape(experts * capacity, model_width)
    weight = down_weight[0]
    own_rows = weight.shape[0]
    factor = 1.0 / math.sqrt(replicas * token_count)
    hidden_grad = lax.dot_general(
        arrived,
        lax.all_gather(weight, "dp", axis=0, tiled=True),
        (((1,), (1,)), ((), ())),
        preferred_element_type=jnp.float32,
    )
    pre_block = pre_act.astype(jnp.float32)
    pre_grad = (hidden_grad * derivative(pre_block)).astype(jnp.bfloat16)
    hidden = activate(pre_block).astype(jnp.bfloat16)
    summed = lax.psum_scatter(
        lax.dot_general(
            hidden, arrived, (((0,), (0,)), ((), ())), preferred_element_type=jnp.float32
        ),
        "dp",
        scatter_dimension=0,
        tiled=True,
    )
    return (pre_grad, (summed * factor).reshape(1, own_rows, model_width))


def solution(mesh):
    placed = (
        P(("dp", "expert"), None),
        P(("dp", "expert"), None),
        P(("dp", "expert"), None),
        P("expert", "dp", None),
    )
    return jax.shard_map(
        body,
        mesh=mesh,
        in_specs=placed,
        out_specs=(P(("dp", "expert"), None), P("expert", "dp", None)),
        check_vma=False,
    )
```

```python
import functools
import math

import jax
import jax.numpy as jnp
from jax import lax
from jax.experimental import pallas as pl
from jax.experimental.pallas import tpu as pltpu
from jax.sharding import PartitionSpec as P

tanh_scale = 0.7978845608028654
cubic_weight = 0.044715
MESH = pl.DeviceIdType.MESH
PAIR = 2
LINE = 4
CUTS = 2
HALVES = 2
PARTS = 2
LANES = 2


def activate(values):
    argument = tanh_scale * (values + cubic_weight * values * values * values)
    return 0.5 * values * (1.0 + jnp.tanh(argument))


def derivative(values):
    tangent = jnp.tanh(tanh_scale * (values + cubic_weight * values * values * values))
    return 0.5 * (1.0 + tangent) + 0.5 * values * (1.0 - tangent * tangent) * tanh_scale * (
        1.0 + 3.0 * cubic_weight * values * values
    )


def kernel(
    experts,
    capacity,
    tokens_hbm,
    route_hbm,
    pre_hbm,
    weight_hbm,
    grad_hbm,
    term_out,
    landed,
    own_tokens,
    own_route,
    their_tokens,
    their_route,
    choose,
    outgoing,
    arrived,
    pre_own,
    pre_theirs,
    lane_in,
    lane_pack,
    lane_got,
    lane_out,
    weights,
    hidden,
    slope,
    partial,
    sums_out,
    sums_in,
    input_sems,
    token_sems,
    dispatch_send,
    dispatch_recv,
    local_sems,
    pre_sems,
    lane_send,
    lane_recv,
    cross_sems,
    weight_send,
    weight_recv,
    sum_send,
    sum_recv,
    grad_sems,
):
    d = lax.axis_index("dp")
    me = lax.axis_index("expert")
    z = lax.div(d, PAIR)
    x = lax.rem(d, PAIR)
    partner = z * PAIR + 1 - x
    rows, width = pre_hbm.shape[0], own_tokens.shape[1]
    block = weight_hbm.shape[0]
    count = own_tokens.shape[0]
    low = z < LINE // 2
    own = LINE - 1
    direct = LINE - LANES
    piece, part_rows, span = block // CUTS, block // PARTS, width // HALVES

    def order(i):
        if i == own:
            return z
        down = LINE - 1 - i
        return jnp.where(
            low, jnp.where(down > z, down, down - 1), jnp.where(i < z, i, i + 1)
        )

    def columns(j, side):
        return pl.ds(pl.multiple_of((j * PAIR + side) * block, block), block)

    def within(cut):
        return pl.ds(cut * piece, piece)

    def across(half):
        return pl.ds(half * span, span)

    def slots(source):
        return pl.ds(pl.multiple_of(source * capacity, capacity), capacity)

    def peer(k):
        return lax.rem(me + k, experts)

    def from_peer(k):
        return lax.rem(me + experts - k, experts)

    route_load = pltpu.make_async_copy(route_hbm, own_route, input_sems.at[0])
    token_load = pltpu.make_async_copy(tokens_hbm, own_tokens, input_sems.at[1])
    weight_own = pltpu.make_async_copy(weight_hbm, weights.at[z], local_sems.at[LINE])
    weight_own.start()
    route_load.start()
    token_load.start()

    barrier = pltpu.get_barrier_semaphore()
    pl.semaphore_signal(barrier, inc=1, device_id={"dp": partner}, device_id_type=MESH)
    for k in range(1, experts):
        pl.semaphore_signal(
            barrier, inc=1, device_id={"expert": peer(k)}, device_id_type=MESH
        )

    @pl.when(z > 0)
    def _():
        pl.semaphore_signal(barrier, inc=1, device_id={"dp": d - PAIR}, device_id_type=MESH)

    @pl.when(z < LINE - 1)
    def _():
        pl.semaphore_signal(barrier, inc=1, device_id={"dp": d + PAIR}, device_id_type=MESH)

    inner = jnp.where((z > 0) & (z < LINE - 1), 2, 1)
    pl.semaphore_wait(barrier, experts + inner)

    def remote(src, dst, send, recv, device):
        return pltpu.make_async_remote_copy(
            src_ref=src, dst_ref=dst, send_sem=send, recv_sem=recv,
            device_id=device, device_id_type=MESH,
        )

    route_copy = remote(
        route_hbm, their_route, token_sems.at[0, HALVES], token_sems.at[1, HALVES],
        {"dp": partner},
    )

    def token_copy(half):
        return remote(
            own_tokens.at[:, across(half)], their_tokens.at[:, across(half)],
            token_sems.at[0, half], token_sems.at[1, half], {"dp": partner},
        )

    def pre_copy(i, cut):
        start = (order(i) * PAIR + 1 - x) * block + cut * piece
        return remote(
            pre_hbm.at[:, pl.ds(pl.multiple_of(start, piece), piece)],
            pre_theirs.at[i, :, within(cut)],
            pre_sems.at[0, i, cut], pre_sems.at[1, i, cut], {"dp": partner},
        )

    def cross(lane):
        return remote(
            lane_pack.at[lane], lane_got.at[lane],
            cross_sems.at[0, lane], cross_sems.at[1, lane], {"dp": partner},
        )

    def part(c):
        return pl.ds(c * part_rows, part_rows)

    def weight_copy(direction, hop, c):
        step = 1 - 2 * direction
        shard = jnp.clip(z - step * hop, 0, LINE - 1)
        return remote(
            weights.at[shard, part(c)], weights.at[shard, part(c)], weight_send.at[direction, hop, c],
            weight_recv.at[direction, hop, c], {"dp": d + step * PAIR},
        )

    def sends(direction, hop):
        if direction == 0:
            return (z >= hop) & (z < LINE - 1)
        return (z <= LINE - 1 - hop) & (z > 0)

    def receives(direction, hop):
        return (z > hop) if direction == 0 else (z < LINE - 1 - hop)

    def weight_start(hop, c):
        for direction in range(2):
            @pl.when(sends(direction, hop))
            def _():
                weight_copy(direction, hop, c).start()

    def weight_arrive(hop, c):
        for direction in range(2):
            @pl.when(receives(direction, hop))
            def _():
                step = 1 - 2 * direction
                shard = jnp.clip(z - step * (hop + 1), 0, LINE - 1)
                remote(
                    weight_hbm.at[part(c)], weights.at[shard, part(c)],
                    weight_send.at[direction, hop, c],
                    weight_recv.at[direction, hop, c], {"dp": partner},
                ).wait_recv()

        if hop < LINE - 2:
            weight_start(hop + 1, c)

    weight_own.wait()
    for c in range(PARTS):
        weight_start(0, c)
    route_copy.start()
    token_load.wait()
    for half in range(HALVES):
        token_copy(half).start()
    for i in range(direct):
        for cut in range(CUTS):
            pre_copy(i, cut).start()

    def own_copy(i):
        return pltpu.make_async_copy(
            pre_hbm.at[:, columns(order(i), x)], pre_own.at[i], local_sems.at[i]
        )

    for i in range(LINE):
        own_copy(i).start()
    earlier = (
        lax.broadcasted_iota(jnp.int32, (count, count), 0)
        < lax.broadcasted_iota(jnp.int32, (count, count), 1)
    ).astype(jnp.float32).astype(jnp.bfloat16)

    def plan(rep, routes):
        names = routes[...]
        named = lax.broadcasted_iota(jnp.int32, (8, count), 0) == names
        onehot = named.astype(jnp.float32)
        before = jnp.dot(
            onehot.astype(jnp.bfloat16), earlier, preferred_element_type=jnp.float32
        )
        position = jnp.sum(onehot * before, axis=0, keepdims=True).astype(jnp.int32)
        slot = lax.broadcasted_iota(jnp.int32, (capacity, count), 0)
        for e in range(experts):
            place = jnp.where(names == e, position, -1)
            choose[rep, e * capacity:(e + 1) * capacity, :] = (
                (slot == place).astype(jnp.float32).astype(jnp.bfloat16)
            )

    def dispatch_copy(rep, k, half):
        return remote(
            outgoing.at[rep, k - 1, :, across(half)],
            arrived.at[rep, slots(me), across(half)],
            dispatch_send.at[rep, k - 1, half],
            dispatch_recv.at[rep, k - 1, half],
            {"expert": peer(k)},
        )

    def dispatch(rep, tokens, half):
        for k in list(range(1, experts)) + [0]:
            rows_out = jnp.dot(
                choose[rep, slots(peer(k)), :], tokens[:, across(half)],
                preferred_element_type=jnp.float32,
            ).astype(jnp.bfloat16)
            if k == 0:
                arrived[rep, slots(me), across(half)] = rows_out
            else:
                outgoing[rep, k - 1, :, across(half)] = rows_out
                dispatch_copy(rep, k, half).start()

    def tokens_arrive(rep, half):
        for k in range(1, experts):
            remote(
                outgoing.at[rep, k - 1, :, across(half)],
                arrived.at[rep, slots(from_peer(k)), across(half)],
                dispatch_send.at[rep, k - 1, half],
                dispatch_recv.at[rep, k - 1, half],
                {"expert": peer(k)},
            ).wait_recv()

    def lane_unit(lane):
        return own - lane

    def lane_columns(lane):
        return columns(order(lane_unit(lane)), 1 - x)

    def lane_target(leg, lane, source):
        if leg == 0:
            return lane_in.at[lane, slots(source)]
        if leg == 1:
            return pre_theirs.at[lane_unit(lane), slots(source)]
        if leg == 2:
            return lane_in.at[LANES + lane, slots(source)]
        return grad_hbm.at[slots(source), lane_columns(lane)]

    def lane_copy(leg, lane, k):
        if leg == 0:
            src = pre_hbm.at[slots(peer(k)), lane_columns(lane)]
        elif leg == 2:
            src = pre_theirs.at[lane_unit(lane), slots(peer(k))]
        else:
            src = lane_out.at[lane + LANES * (leg // 2), k]
        return remote(
            src, lane_target(leg, lane, me), lane_send.at[leg, lane, k - 1],
            lane_recv.at[leg, lane, k - 1], {"expert": peer(k)},
        )

    def lane_arrive(leg, lane):
        for k in range(1, experts):
            remote(
                lane_out.at[lane, k], lane_target(leg, lane, from_peer(k)),
                lane_send.at[leg, lane, k - 1], lane_recv.at[leg, lane, k - 1],
                {"expert": peer(k)},
            ).wait_recv()

    def lane_local(lane):
        return pltpu.make_async_copy(
            pre_hbm.at[slots(me), lane_columns(lane)], lane_in.at[lane, slots(me)],
            local_sems.at[LINE + 1 + lane],
        )

    def lane_home(lane):
        return pltpu.make_async_copy(
            lane_out.at[LANES + lane, 0], grad_hbm.at[slots(me), lane_columns(lane)],
            local_sems.at[LINE + 1 + LANES + lane],
        )

    def gather(way, lane):
        if way == 0:
            lane_local(lane).wait()
        lane_arrive(2 * way, lane)
        at = LANES * way + lane
        lane_pack[at] = lax.dot_general(
            choose[way], lane_in[at], (((0,), (0,)), ((), ())),
            preferred_element_type=jnp.float32,
        ).astype(jnp.bfloat16)
        cross(at).start()

    def spread(way, lane):
        at = LANES * way + lane
        cross(at).wait_recv()
        for k in list(range(1, experts)) + [0]:
            rows_out = jnp.dot(
                choose[1 - way, slots(peer(k)), :], lane_got[at],
                preferred_element_type=jnp.float32,
            ).astype(jnp.bfloat16)
            if way == 0 and k == 0:
                pre_theirs[lane_unit(lane), slots(me), :] = rows_out
            else:
                lane_out[at, k] = rows_out
                if k == 0:
                    lane_home(lane).start()
                else:
                    lane_copy(2 * way + 1, lane, k).start()

    strip = 64

    def activate_rows(rep, i, source, cut):
        at_columns = within(cut)

        @pl.loop(0, rows // (2 * strip))
        def _(t):
            for half in range(2):
                at = pl.ds(pl.multiple_of(t * 2 * strip + half * strip, strip), strip)
                v = source[i, at, at_columns].astype(jnp.float32)
                square = v * v
                tangent = jnp.tanh(tanh_scale * v * (1.0 + cubic_weight * square))
                gate = 0.5 * (1.0 + tangent)
                slope[rep, i, at, at_columns] = gate + 0.5 * v * (
                    1.0 - tangent * tangent
                ) * tanh_scale * (1.0 + 3.0 * cubic_weight * square)
                hidden[rep, i, at, at_columns] = (v * gate).astype(jnp.bfloat16)

    def activate_own(i):
        own_copy(i).wait()
        for cut in range(CUTS):
            activate_rows(0, i, pre_own, cut)

    def activate_theirs(i, cut):
        if i < direct:
            pre_copy(i, cut).wait_recv()
        activate_rows(1, i, pre_theirs, cut)

    def term(i, cut, half):
        at, wide = within(cut), across(half)
        total = lax.dot_general(
            hidden[0, i, :, at], arrived[0, :, wide], (((0,), (0,)), ((), ())),
            preferred_element_type=jnp.float32,
        )
        partial[i, at, wide] = total + lax.dot_general(
            hidden[1, i, :, at], arrived[1, :, wide], (((0,), (0,)), ((), ())),
            preferred_element_type=jnp.float32,
        )

    def terms(i):
        for cut in range(CUTS):
            for half in range(HALVES):
                term(i, cut, half)
            if i < own:
                begin(i, cut)

    def pieces(stage):
        return range(HALVES) if stage == 0 else (None,)

    def sum_copy(direction, stage, cut, half, i=0):
        at = within(cut)
        wide = pl.ds(0, width) if half is None else across(half)
        target = landed.at[direction] if stage == LINE - 2 else sums_in.at[direction, stage]
        slot = (direction, stage, cut, half or 0)
        return remote(
            sums_out.at[i, at, wide], target.at[at, wide],
            sum_send.at[slot], sum_recv.at[slot], {"dp": d + (1 - 2 * direction) * PAIR},
        )

    def toward(i, direction, ends):
        j = order(i)
        away = (j > z) if direction == 0 else (j < z)
        first = (z == 0) if direction == 0 else (z == LINE - 1)
        return away & first if ends else away & jnp.logical_not(first)

    def begin(i, cut, half=None):
        at = within(cut)
        wide = pl.ds(0, width) if half is None else across(half)
        for direction in range(2):
            @pl.when(toward(i, direction, True))
            def _():
                sums_out[i, at, wide] = partial[i, at, wide].astype(jnp.bfloat16)
                sum_copy(direction, i, cut, half, i).start()

    def forward(i, cut):
        at = within(cut)
        stage = min(i + 1, LINE - 2)
        for direction in range(2):
            @pl.when(toward(i, direction, False))
            def _():
                for half in pieces(stage - 1):
                    sum_copy(direction, stage - 1, cut, half).wait_recv()
                sums_out[i, at, :] = (
                    partial[i, at, :]
                    + sums_in[direction, stage - 1, at, :].astype(jnp.float32)
                ).astype(jnp.bfloat16)
                sum_copy(direction, stage, cut, None, i).start()

    def grad_copy(i):
        return remote(
            pre_theirs.at[i], grad_hbm.at[:, columns(order(i), x)],
            grad_sems.at[0, i], grad_sems.at[1, i], {"dp": partner},
        )

    def grad_arrive(i):
        return remote(
            pre_theirs.at[i], grad_hbm.at[:, columns(order(i), 1 - x)],
            grad_sems.at[0, i], grad_sems.at[1, i], {"dp": partner},
        )

    def grad_write(i):
        return pltpu.make_async_copy(
            pre_own.at[i], grad_hbm.at[:, columns(order(i), x)], grad_sems.at[2, i]
        )

    tile = 256

    def differentiate(rep, i):
        j = order(i)
        result = pre_theirs if rep == 1 else pre_own

        @pl.loop(0, rows // tile)
        def _(t):
            at = pl.ds(pl.multiple_of(t * tile, tile), tile)
            product = lax.dot_general(
                arrived[rep, at, :], weights[j], (((1,), (1,)), ((), ())),
                preferred_element_type=jnp.float32,
            )
            result[i, at, :] = (product * slope[rep, i, at, :]).astype(jnp.bfloat16)

        if rep == 0:
            grad_write(i).start()
        elif i < direct:
            grad_copy(i).start()
        else:
            for k in range(1, experts):
                lane_copy(2, own - i, k).start()
            lane_in[LANES + own - i, slots(me), :] = pre_theirs[i, slots(me), :]

    route_load.wait()
    plan(0, own_route)
    dispatch(0, own_tokens, 0)
    activate_own(0)
    activate_own(1)
    route_copy.wait_recv()
    plan(1, their_route)
    token_copy(0).wait_recv()
    dispatch(1, their_tokens, 0)
    dispatch(0, own_tokens, 1)
    activate_own(2)
    weight_arrive(0, 0)
    token_copy(1).wait_recv()
    dispatch(1, their_tokens, 1)
    for lane in range(LANES):
        lane_local(lane).start()
        for k in range(1, experts):
            lane_copy(0, lane, k).start()
    activate_own(own)
    for rep in range(2):
        tokens_arrive(rep, 0)
    for cut in range(CUTS):
        activate_theirs(0, cut)
        term(0, cut, 0)
        begin(0, cut, 0)
    weight_arrive(0, 1)
    for rep in range(2):
        tokens_arrive(rep, 1)
    for cut in range(CUTS):
        term(0, cut, 1)
        begin(0, cut, 1)
    differentiate(0, own)
    differentiate(0, own - 1)
    gather(0, 0)
    activate_theirs(1, 0)
    weight_arrive(1, 0)
    gather(0, 1)
    activate_theirs(1, 1)
    forward(0, 0)
    terms(1)
    spread(0, 0)
    forward(0, 1)
    weight_arrive(1, 1)
    spread(0, 1)
    differentiate(1, 1)
    differentiate(0, 1)
    lane_arrive(1, 0)
    for cut in range(CUTS):
        activate_theirs(own, cut)
    differentiate(1, own)
    terms(own)
    term_copy = pltpu.make_async_copy(
        partial.at[own], term_out, local_sems.at[LINE + 1 + 2 * LANES]
    )
    term_copy.start()
    lane_arrive(1, 1)
    for cut in range(CUTS):
        activate_theirs(own - 1, cut)
    terms(own - 1)
    differentiate(1, own - 1)
    forward(1, 0)
    forward(2, 0)
    weight_arrive(2, 0)
    gather(1, 0)
    gather(1, 1)
    forward(1, 1)
    forward(2, 1)
    weight_arrive(2, 1)
    differentiate(1, 0)
    differentiate(0, 0)
    for lane in range(LANES):
        spread(1, lane)

    for lane in range(LANES):
        lane_arrive(3, lane)
        lane_home(lane).wait()
    for i in range(LINE):
        if i < direct:
            grad_arrive(i).wait_recv()
        grad_write(i).wait()
    term_copy.wait()
    for direction in range(2):
        @pl.when(receives(direction, 0))
        def _():
            for cut in range(CUTS):
                sum_copy(direction, LINE - 2, cut, None).wait_recv()
    route_copy.wait_send()
    for half in range(HALVES):
        token_copy(half).wait_send()
    for i in range(direct):
        for cut in range(CUTS):
            pre_copy(i, cut).wait_send()
        grad_copy(i).wait_send()
    for lane in range(LANES):
        cross(lane).wait_send()
        cross(LANES + lane).wait_send()
    for k in range(1, experts):
        for leg in range(4):
            for lane in range(LANES):
                lane_copy(leg, lane, k).wait_send()
        for rep in range(2):
            for half in range(HALVES):
                dispatch_copy(rep, k, half).wait_send()
    for hop in range(LINE - 1):
        for direction in range(2):
            @pl.when(sends(direction, hop))
            def _():
                for c in range(PARTS):
                    weight_copy(direction, hop, c).wait_send()
    for stage in range(LINE - 1):
        for direction in range(2):
            sent = (z <= stage) if direction == 0 else (z >= LINE - 1 - stage)
            inside = (z < LINE - 1) if direction == 0 else (z > 0)

            @pl.when(sent & inside)
            def _():
                for cut in range(CUTS):
                    for half in pieces(stage):
                        sum_copy(direction, stage, cut, half).wait_send()


def finish(factor, grad_ref, term_ref, landed_ref, grad_hbm, dw_hbm, summed, sems):
    z = lax.div(lax.axis_index("dp"), PAIR)
    rows, block = grad_ref.shape[0], term_ref.shape[0]
    steps = 4

    def grad_write(c):
        at = pl.ds(c * (rows // steps), rows // steps)
        return pltpu.make_async_copy(grad_ref.at[at], grad_hbm.at[at], sems.at[0, c])

    def sum_write(c):
        at = pl.ds(c * (block // steps), block // steps)
        return pltpu.make_async_copy(summed.at[at], dw_hbm.at[at], sems.at[1, c])

    for c in range(steps):
        grad_write(c).start()
    for c in range(steps):
        at = pl.ds(c * (block // steps), block // steps)
        up = jnp.where(z > 0, landed_ref[0, at, :].astype(jnp.float32), 0.0)
        down = jnp.where(z < LINE - 1, landed_ref[1, at, :].astype(jnp.float32), 0.0)
        summed[at, :] = (term_ref[at, :] + up + down) * factor
        sum_write(c).start()
    for c in range(steps):
        grad_write(c).wait()
        sum_write(c).wait()


def fused(out_grad, expert_of, pre_act, down_weight):
    experts = lax.axis_size("expert")
    replicas = lax.axis_size("dp")
    count, width = out_grad.shape
    rows, units = pre_act.shape
    block = down_weight.shape[1]
    capacity = count // 2
    factor = 1.0 / math.sqrt(replicas * count)
    half, full = jnp.bfloat16, jnp.float32
    hbm = pl.BlockSpec(memory_space=pltpu.HBM)
    anywhere = pl.BlockSpec(memory_space=pl.ANY)
    dma = pltpu.SemaphoreType.DMA
    placed = pl.pallas_call(
        functools.partial(kernel, experts, capacity),
        out_shape=(
            pltpu.VMEM((rows, units), half),
            pltpu.VMEM((block, width), full),
            pltpu.VMEM((2, block, width), half),
        ),
        in_specs=[hbm, hbm, hbm, hbm],
        out_specs=(anywhere, anywhere, anywhere),
        scratch_shapes=[
            pltpu.VMEM((count, width), half),
            pltpu.VMEM((1, count), jnp.int32),
            pltpu.VMEM((count, width), half),
            pltpu.VMEM((1, count), jnp.int32),
            pltpu.VMEM((2, experts * capacity, count), half),
            pltpu.VMEM((2, experts - 1, capacity, width), half),
            pltpu.VMEM((2, rows, width), half),
            pltpu.VMEM((LINE, rows, block), half),
            pltpu.VMEM((LINE, rows, block), half),
            pltpu.VMEM((2 * LANES, rows, block), half),
            pltpu.VMEM((2 * LANES, count, block), half),
            pltpu.VMEM((2 * LANES, count, block), half),
            pltpu.VMEM((2 * LANES, experts, capacity, block), half),
            pltpu.VMEM((LINE, block, width), half),
            pltpu.VMEM((2, LINE, rows, block), half),
            pltpu.VMEM((2, LINE, rows, block), full),
            pltpu.VMEM((LINE, block, width), full),
            pltpu.VMEM((LINE - 1, block, width), half),
            pltpu.VMEM((2, LINE - 2, block, width), half),
            dma((2,)),
            dma((2, HALVES + 1)),
            dma((2, experts - 1, HALVES)),
            dma((2, experts - 1, HALVES)),
            dma((LINE + 2 + 2 * LANES,)),
            dma((2, LINE - LANES, CUTS)),
            dma((4, LANES, experts - 1)),
            dma((4, LANES, experts - 1)),
            dma((2, 2 * LANES)),
            dma((2, LINE - 1, PARTS)),
            dma((2, LINE - 1, PARTS)),
            dma((2, LINE - 1, CUTS, HALVES)),
            dma((2, LINE - 1, CUTS, HALVES)),
            dma((3, LINE)),
        ],
        compiler_params=pltpu.CompilerParams(
            collective_id=0, has_side_effects=True, vmem_limit_bytes=51 * 1024 * 1024
        ),
    )(*(
        pltpu.with_memory_space_constraint(array, pltpu.HBM)
        for array in (out_grad, expert_of.reshape(1, count), pre_act, down_weight[0])
    ))
    vmem = pl.BlockSpec(memory_space=pltpu.VMEM)
    pre_grad, summed = pl.pallas_call(
        functools.partial(finish, factor),
        out_shape=(
            jax.ShapeDtypeStruct((rows, units), half),
            jax.ShapeDtypeStruct((block, width), full),
        ),
        in_specs=[vmem, vmem, vmem],
        out_specs=(hbm, hbm),
        scratch_shapes=[pltpu.VMEM((block, width), full), dma((2, 4))],
        compiler_params=pltpu.CompilerParams(vmem_limit_bytes=16 * 1024 * 1024),
    )(*placed)
    return pre_grad, summed.reshape(1, block, width)


def body(out_grad, expert_of, pre_act, down_weight):
    experts = lax.axis_size("expert")
    replicas = lax.axis_size("dp")
    if replicas == PAIR * LINE and experts <= 8:
        return fused(out_grad, expert_of, pre_act, down_weight)
    token_count = out_grad.shape[0]
    model_width = out_grad.shape[1]
    capacity = token_count // 2
    routed = expert_of[:, 0]
    onehot = (routed[:, None] == jnp.arange(experts, dtype=jnp.int32)[None, :]).astype(jnp.int32)
    position = jnp.sum((jnp.cumsum(onehot, axis=0) - onehot) * onehot, axis=1)
    target = routed * capacity + position
    outgoing = jnp.zeros((experts * capacity, model_width), jnp.bfloat16).at[target].set(out_grad)
    arrived = lax.all_to_all(
        outgoing.reshape(experts, capacity, model_width),
        "expert",
        split_axis=0,
        concat_axis=0,
        tiled=True,
    )
    arrived = arrived.reshape(experts * capacity, model_width)
    weight = down_weight[0]
    own_rows = weight.shape[0]
    factor = 1.0 / math.sqrt(replicas * token_count)
    hidden_grad = lax.dot_general(
        arrived,
        lax.all_gather(weight, "dp", axis=0, tiled=True),
        (((1,), (1,)), ((), ())),
        preferred_element_type=jnp.float32,
    )
    pre_block = pre_act.astype(jnp.float32)
    pre_grad = (hidden_grad * derivative(pre_block)).astype(jnp.bfloat16)
    hidden = activate(pre_block).astype(jnp.bfloat16)
    summed = lax.psum_scatter(
        lax.dot_general(
            hidden, arrived, (((0,), (0,)), ((), ())), preferred_element_type=jnp.float32
        ),
        "dp",
        scatter_dimension=0,
        tiled=True,
    )
    return (pre_grad, (summed * factor).reshape(1, own_rows, model_width))


def solution(mesh):
    placed = (
        P(("dp", "expert"), None),
        P(("dp", "expert"), None),
        P(("dp", "expert"), None),
        P("expert", "dp", None),
    )
    return jax.shard_map(
        body,
        mesh=mesh,
        in_specs=placed,
        out_specs=(P(("dp", "expert"), None), P("expert", "dp", None)),
        check_vma=False,
    )
```

```python
import functools
import math

import jax
import jax.numpy as jnp
from jax import lax
from jax.experimental import pallas as pl
from jax.experimental.pallas import tpu as pltpu
from jax.sharding import PartitionSpec as P

tanh_scale = 0.7978845608028654
cubic_weight = 0.044715
MESH = pl.DeviceIdType.MESH
PAIR = 2
LINE = 4
CUTS = 2
HALVES = 2
PARTS = 2
LANES = 2


def activate(values):
    argument = tanh_scale * (values + cubic_weight * values * values * values)
    return 0.5 * values * (1.0 + jnp.tanh(argument))


def derivative(values):
    tangent = jnp.tanh(tanh_scale * (values + cubic_weight * values * values * values))
    return 0.5 * (1.0 + tangent) + 0.5 * values * (1.0 - tangent * tangent) * tanh_scale * (
        1.0 + 3.0 * cubic_weight * values * values
    )


def kernel(
    experts,
    capacity,
    tokens_hbm,
    route_hbm,
    pre_hbm,
    weight_hbm,
    grad_hbm,
    term_out,
    landed,
    own_tokens,
    own_route,
    their_tokens,
    their_route,
    choose,
    outgoing,
    arrived,
    pre_own,
    pre_theirs,
    lane_in,
    lane_pack,
    lane_got,
    lane_out,
    weights,
    hidden,
    slope,
    partial,
    sums_out,
    sums_in,
    input_sems,
    token_sems,
    dispatch_send,
    dispatch_recv,
    local_sems,
    pre_sems,
    lane_send,
    lane_recv,
    cross_sems,
    weight_send,
    weight_recv,
    sum_send,
    sum_recv,
    grad_sems,
):
    d = lax.axis_index("dp")
    me = lax.axis_index("expert")
    z = lax.div(d, PAIR)
    x = lax.rem(d, PAIR)
    partner = z * PAIR + 1 - x
    rows, width = pre_hbm.shape[0], own_tokens.shape[1]
    block = weight_hbm.shape[0]
    count = own_tokens.shape[0]
    low = z < LINE // 2
    own = LINE - 1
    direct = LINE - LANES
    piece, part_rows, span = block // CUTS, block // PARTS, width // HALVES

    def order(i):
        if i == own:
            return z
        down = LINE - 1 - i
        return jnp.where(
            low, jnp.where(down > z, down, down - 1), jnp.where(i < z, i, i + 1)
        )

    def columns(j, side):
        return pl.ds(pl.multiple_of((j * PAIR + side) * block, block), block)

    def within(cut):
        return pl.ds(cut * piece, piece)

    def across(half):
        return pl.ds(half * span, span)

    def slots(source):
        return pl.ds(pl.multiple_of(source * capacity, capacity), capacity)

    def peer(k):
        return lax.rem(me + k, experts)

    def from_peer(k):
        return lax.rem(me + experts - k, experts)

    route_load = pltpu.make_async_copy(route_hbm, own_route, input_sems.at[0])
    token_load = pltpu.make_async_copy(tokens_hbm, own_tokens, input_sems.at[1])
    weight_own = pltpu.make_async_copy(weight_hbm, weights.at[z], local_sems.at[LINE])
    weight_own.start()
    route_load.start()
    token_load.start()

    barrier = pltpu.get_barrier_semaphore()
    pl.semaphore_signal(barrier, inc=1, device_id={"dp": partner}, device_id_type=MESH)
    for k in range(1, experts):
        pl.semaphore_signal(
            barrier, inc=1, device_id={"expert": peer(k)}, device_id_type=MESH
        )

    @pl.when(z > 0)
    def _():
        pl.semaphore_signal(barrier, inc=1, device_id={"dp": d - PAIR}, device_id_type=MESH)

    @pl.when(z < LINE - 1)
    def _():
        pl.semaphore_signal(barrier, inc=1, device_id={"dp": d + PAIR}, device_id_type=MESH)

    inner = jnp.where((z > 0) & (z < LINE - 1), 2, 1)
    pl.semaphore_wait(barrier, experts + inner)

    def remote(src, dst, send, recv, device):
        return pltpu.make_async_remote_copy(
            src_ref=src, dst_ref=dst, send_sem=send, recv_sem=recv,
            device_id=device, device_id_type=MESH,
        )

    route_copy = remote(
        route_hbm, their_route, token_sems.at[0], token_sems.at[1],
        {"dp": partner},
    )

    def token_copy(half):
        return remote(
            own_tokens.at[:, across(half)], their_tokens.at[:, across(half)],
            token_sems.at[2], token_sems.at[3 + half], {"dp": partner},
        )

    def pre_copy(i, cut):
        start = (order(i) * PAIR + 1 - x) * block + cut * piece
        return remote(
            pre_hbm.at[:, pl.ds(pl.multiple_of(start, piece), piece)],
            pre_theirs.at[i, :, within(cut)],
            pre_sems.at[0], pre_sems.at[1 + i * CUTS + cut], {"dp": partner},
        )

    def cross(lane):
        return remote(
            lane_pack.at[lane], lane_got.at[lane],
            cross_sems.at[0], cross_sems.at[1 + lane], {"dp": partner},
        )

    def part(c):
        return pl.ds(c * part_rows, part_rows)

    def weight_copy(direction, hop, c):
        step = 1 - 2 * direction
        shard = jnp.clip(z - step * hop, 0, LINE - 1)
        return remote(
            weights.at[shard, part(c)], weights.at[shard, part(c)], weight_send.at[direction],
            weight_recv.at[shard, c], {"dp": d + step * PAIR},
        )

    def sends(direction, hop):
        if direction == 0:
            return (z >= hop) & (z < LINE - 1)
        return (z <= LINE - 1 - hop) & (z > 0)

    def receives(direction, hop):
        return (z > hop) if direction == 0 else (z < LINE - 1 - hop)

    def weight_start(hop, c):
        for direction in range(2):
            @pl.when(sends(direction, hop))
            def _():
                weight_copy(direction, hop, c).start()

    def weight_arrive(hop, c):
        for direction in range(2):
            @pl.when(receives(direction, hop))
            def _():
                step = 1 - 2 * direction
                shard = jnp.clip(z - step * (hop + 1), 0, LINE - 1)
                remote(
                    weight_hbm.at[part(c)], weights.at[shard, part(c)],
                    weight_send.at[direction], weight_recv.at[shard, c], {"dp": partner},
                ).wait_recv()

        if hop < LINE - 2:
            weight_start(hop + 1, c)

    weight_own.wait()
    for c in range(PARTS):
        weight_start(0, c)
    route_copy.start()
    token_load.wait()
    for half in range(HALVES):
        token_copy(half).start()
    for i in range(direct):
        for cut in range(CUTS):
            pre_copy(i, cut).start()

    def own_copy(i):
        return pltpu.make_async_copy(
            pre_hbm.at[:, columns(order(i), x)], pre_own.at[i], local_sems.at[i]
        )

    for i in range(LINE):
        own_copy(i).start()
    earlier = (
        lax.broadcasted_iota(jnp.int32, (count, count), 0)
        < lax.broadcasted_iota(jnp.int32, (count, count), 1)
    ).astype(jnp.float32).astype(jnp.bfloat16)

    def plan(rep, routes):
        names = routes[...]
        named = lax.broadcasted_iota(jnp.int32, (8, count), 0) == names
        onehot = named.astype(jnp.float32)
        before = jnp.dot(
            onehot.astype(jnp.bfloat16), earlier, preferred_element_type=jnp.float32
        )
        position = jnp.sum(onehot * before, axis=0, keepdims=True).astype(jnp.int32)
        slot = lax.broadcasted_iota(jnp.int32, (capacity, count), 0)
        for e in range(experts):
            place = jnp.where(names == e, position, -1)
            choose[rep, e * capacity:(e + 1) * capacity, :] = (
                (slot == place).astype(jnp.float32).astype(jnp.bfloat16)
            )

    def dispatch_copy(rep, k, half):
        return remote(
            outgoing.at[rep, k - 1, :, across(half)],
            arrived.at[rep, slots(me), across(half)],
            dispatch_send.at[0],
            dispatch_recv.at[half],
            {"expert": peer(k)},
        )

    def dispatch(rep, tokens, half):
        for k in list(range(1, experts)) + [0]:
            rows_out = jnp.dot(
                choose[rep, slots(peer(k)), :], tokens[:, across(half)],
                preferred_element_type=jnp.float32,
            ).astype(jnp.bfloat16)
            if k == 0:
                arrived[rep, slots(me), across(half)] = rows_out
            else:
                outgoing[rep, k - 1, :, across(half)] = rows_out
                dispatch_copy(rep, k, half).start()

    peers = pl.ds(0, (experts - 1) * capacity)

    def tokens_arrive(half):
        came = arrived.at[:, peers, across(half)]
        remote(
            came, came, dispatch_send.at[0], dispatch_recv.at[half], {"expert": peer(1)}
        ).wait_recv()

    def lane_unit(lane):
        return own - lane

    def lane_columns(lane):
        return columns(order(lane_unit(lane)), 1 - x)

    def lane_target(leg, lane, source):
        if leg == 0:
            return lane_in.at[lane, slots(source)]
        if leg == 1:
            return pre_theirs.at[lane_unit(lane), slots(source)]
        if leg == 2:
            return lane_in.at[LANES + lane, slots(source)]
        return grad_hbm.at[slots(source), lane_columns(lane)]

    def lane_copy(leg, lane, k):
        if leg == 0:
            src = pre_hbm.at[slots(peer(k)), lane_columns(lane)]
        elif leg == 2:
            src = pre_theirs.at[lane_unit(lane), slots(peer(k))]
        else:
            src = lane_out.at[lane + LANES * (leg // 2), k]
        return remote(
            src, lane_target(leg, lane, me), lane_send.at[leg // 2], lane_recv.at[leg, lane],
            {"expert": peer(k)},
        )

    def lane_arrive(leg, lane):
        came = lane_in.at[lane, peers]
        remote(
            came, came, lane_send.at[0], lane_recv.at[leg, lane], {"expert": peer(1)}
        ).wait_recv()

    def lane_local(lane):
        return pltpu.make_async_copy(
            pre_hbm.at[slots(me), lane_columns(lane)], lane_in.at[lane, slots(me)],
            local_sems.at[LINE + 1 + lane],
        )

    def lane_home(lane):
        return pltpu.make_async_copy(
            lane_out.at[LANES + lane, 0], grad_hbm.at[slots(me), lane_columns(lane)],
            local_sems.at[LINE + 1 + LANES],
        )

    def gather(way, lane):
        if way == 0:
            lane_local(lane).wait()
        lane_arrive(2 * way, lane)
        at = LANES * way + lane
        lane_pack[at] = lax.dot_general(
            choose[way], lane_in[at], (((0,), (0,)), ((), ())),
            preferred_element_type=jnp.float32,
        ).astype(jnp.bfloat16)
        cross(at).start()

    def spread(way, lane):
        at = LANES * way + lane
        cross(at).wait_recv()
        for k in list(range(1, experts)) + [0]:
            rows_out = jnp.dot(
                choose[1 - way, slots(peer(k)), :], lane_got[at],
                preferred_element_type=jnp.float32,
            ).astype(jnp.bfloat16)
            if way == 0 and k == 0:
                pre_theirs[lane_unit(lane), slots(me), :] = rows_out
            else:
                lane_out[at, k] = rows_out
                if k == 0:
                    lane_home(lane).start()
                else:
                    lane_copy(2 * way + 1, lane, k).start()

    strip = 64

    def activate_rows(rep, i, source, cut):
        at_columns = within(cut)

        @pl.loop(0, rows // (2 * strip))
        def _(t):
            for half in range(2):
                at = pl.ds(pl.multiple_of(t * 2 * strip + half * strip, strip), strip)
                v = source[i, at, at_columns].astype(jnp.float32)
                square = v * v
                tangent = jnp.tanh(tanh_scale * v * (1.0 + cubic_weight * square))
                gate = 0.5 * (1.0 + tangent)
                slope[rep, i, at, at_columns] = gate + 0.5 * v * (
                    1.0 - tangent * tangent
                ) * tanh_scale * (1.0 + 3.0 * cubic_weight * square)
                hidden[rep, i, at, at_columns] = (v * gate).astype(jnp.bfloat16)

    def activate_own(i):
        own_copy(i).wait()
        for cut in range(CUTS):
            activate_rows(0, i, pre_own, cut)

    def activate_theirs(i, cut):
        if i < direct:
            pre_copy(i, cut).wait_recv()
        activate_rows(1, i, pre_theirs, cut)

    def term(i, cut, half):
        at, wide = within(cut), across(half)
        total = lax.dot_general(
            hidden[0, i, :, at], arrived[0, :, wide], (((0,), (0,)), ((), ())),
            preferred_element_type=jnp.float32,
        )
        partial[i, at, wide] = total + lax.dot_general(
            hidden[1, i, :, at], arrived[1, :, wide], (((0,), (0,)), ((), ())),
            preferred_element_type=jnp.float32,
        )

    def terms(i):
        for cut in range(CUTS):
            for half in range(HALVES):
                term(i, cut, half)
            if i < own:
                begin(i, cut)

    def pieces(stage):
        return range(HALVES) if stage == 0 else (None,)

    def sum_copy(direction, stage, cut, half, i=0):
        at = within(cut)
        wide = pl.ds(0, width) if half is None else across(half)
        target = landed.at[direction] if stage == LINE - 2 else sums_in.at[direction, stage]
        if stage == 0:
            slot = cut * HALVES + half
        else:
            slot = CUTS * HALVES + (cut if stage == 1 else CUTS)
        return remote(
            sums_out.at[i, at, wide], target.at[at, wide], sum_send.at[direction],
            sum_recv.at[direction, slot], {"dp": d + (1 - 2 * direction) * PAIR},
        )

    def toward(i, direction, ends):
        j = order(i)
        away = (j > z) if direction == 0 else (j < z)
        first = (z == 0) if direction == 0 else (z == LINE - 1)
        return away & first if ends else away & jnp.logical_not(first)

    def begin(i, cut, half=None):
        at = within(cut)
        wide = pl.ds(0, width) if half is None else across(half)
        for direction in range(2):
            @pl.when(toward(i, direction, True))
            def _():
                sums_out[i, at, wide] = partial[i, at, wide].astype(jnp.bfloat16)
                sum_copy(direction, i, cut, half, i).start()

    def forward(i, cut):
        at = within(cut)
        stage = min(i + 1, LINE - 2)
        for direction in range(2):
            @pl.when(toward(i, direction, False))
            def _():
                for half in pieces(stage - 1):
                    sum_copy(direction, stage - 1, cut, half).wait_recv()
                sums_out[i, at, :] = (
                    partial[i, at, :]
                    + sums_in[direction, stage - 1, at, :].astype(jnp.float32)
                ).astype(jnp.bfloat16)
                sum_copy(direction, stage, cut, None, i).start()

    def grad_copy(i):
        return remote(
            pre_theirs.at[i], grad_hbm.at[:, columns(order(i), x)],
            grad_sems.at[0], grad_sems.at[1], {"dp": partner},
        )

    def grad_write(i):
        return pltpu.make_async_copy(
            pre_own.at[i], grad_hbm.at[:, columns(order(i), x)], grad_sems.at[2]
        )

    tile = 256

    def differentiate(rep, i):
        j = order(i)
        result = pre_theirs if rep == 1 else pre_own

        @pl.loop(0, rows // tile)
        def _(t):
            at = pl.ds(pl.multiple_of(t * tile, tile), tile)
            product = lax.dot_general(
                arrived[rep, at, :], weights[j], (((1,), (1,)), ((), ())),
                preferred_element_type=jnp.float32,
            )
            result[i, at, :] = (product * slope[rep, i, at, :]).astype(jnp.bfloat16)

        if rep == 0:
            grad_write(i).start()
        elif i < direct:
            grad_copy(i).start()
        else:
            for k in range(1, experts):
                lane_copy(2, own - i, k).start()
            lane_in[LANES + own - i, slots(me), :] = pre_theirs[i, slots(me), :]

    route_load.wait()
    plan(0, own_route)
    dispatch(0, own_tokens, 0)
    activate_own(0)
    activate_own(1)
    route_copy.wait_recv()
    plan(1, their_route)
    token_copy(0).wait_recv()
    dispatch(1, their_tokens, 0)
    dispatch(0, own_tokens, 1)
    activate_own(2)
    weight_arrive(0, 0)
    token_copy(1).wait_recv()
    dispatch(1, their_tokens, 1)
    for lane in range(LANES):
        lane_local(lane).start()
        for k in range(1, experts):
            lane_copy(0, lane, k).start()
    activate_own(own)
    tokens_arrive(0)
    for cut in range(CUTS):
        activate_theirs(0, cut)
        term(0, cut, 0)
        begin(0, cut, 0)
    weight_arrive(0, 1)
    tokens_arrive(1)
    for cut in range(CUTS):
        term(0, cut, 1)
        begin(0, cut, 1)
    differentiate(0, own)
    differentiate(0, own - 1)
    gather(0, 0)
    activate_theirs(1, 0)
    weight_arrive(1, 0)
    gather(0, 1)
    activate_theirs(1, 1)
    forward(0, 0)
    terms(1)
    spread(0, 0)
    forward(0, 1)
    weight_arrive(1, 1)
    spread(0, 1)
    differentiate(1, 1)
    differentiate(0, 1)
    lane_arrive(1, 0)
    for cut in range(CUTS):
        activate_theirs(own, cut)
    differentiate(1, own)
    terms(own)
    term_copy = pltpu.make_async_copy(
        partial.at[own], term_out, local_sems.at[LINE + 2 + LANES]
    )
    term_copy.start()
    lane_arrive(1, 1)
    for cut in range(CUTS):
        activate_theirs(own - 1, cut)
    terms(own - 1)
    differentiate(1, own - 1)
    forward(1, 0)
    forward(2, 0)
    weight_arrive(2, 0)
    gather(1, 0)
    gather(1, 1)
    forward(1, 1)
    forward(2, 1)
    weight_arrive(2, 1)
    differentiate(1, 0)
    differentiate(0, 0)
    for lane in range(LANES):
        spread(1, lane)

    for lane in range(LANES):
        lane_arrive(3, lane)
    home = lane_out.at[pl.ds(LANES, LANES), 0]
    pltpu.make_async_copy(home, home, local_sems.at[LINE + 1 + LANES]).wait()
    units = pre_theirs.at[pl.ds(0, direct)]
    returned = remote(units, units, grad_sems.at[0], grad_sems.at[1], {"dp": partner})
    returned.wait_recv()
    pltpu.make_async_copy(pre_own, pre_own, grad_sems.at[2]).wait()
    term_copy.wait()
    for direction in range(2):
        @pl.when(receives(direction, 0))
        def _():
            whole = landed.at[direction]
            remote(
                whole, whole, sum_send.at[direction],
                sum_recv.at[direction, CUTS * HALVES + CUTS], {"dp": partner},
            ).wait_recv()

    route_copy.wait_send()
    remote(
        own_tokens, their_tokens, token_sems.at[2], token_sems.at[3], {"dp": partner}
    ).wait_send()
    remote(units, units, pre_sems.at[0], pre_sems.at[1], {"dp": partner}).wait_send()
    returned.wait_send()
    remote(
        lane_pack, lane_got, cross_sems.at[0], cross_sems.at[1], {"dp": partner}
    ).wait_send()
    remote(
        outgoing, outgoing, dispatch_send.at[0], dispatch_recv.at[0], {"expert": peer(1)}
    ).wait_send()
    lanes_sent = lane_in.at[:, peers]
    for way in range(2):
        remote(
            lanes_sent, lanes_sent, lane_send.at[way], lane_recv.at[0, 0], {"expert": peer(1)}
        ).wait_send()
    for n in range(1, LINE):
        for direction in range(2):
            @pl.when(z == (n - 1 if direction == 0 else LINE - n))
            def _():
                shards = weights.at[pl.ds(0, n)]
                remote(
                    shards, shards, weight_send.at[direction], weight_recv.at[0, 0],
                    {"dp": partner},
                ).wait_send()

            @pl.when(z == (LINE - 1 - n if direction == 0 else n))
            def _():
                sent = sums_out.at[pl.ds(0, n)]
                remote(
                    sent, sent, sum_send.at[direction], sum_recv.at[direction, 0],
                    {"dp": partner},
                ).wait_send()


def finish(factor, grad_ref, term_ref, landed_ref, grad_hbm, dw_hbm, summed, sems):
    z = lax.div(lax.axis_index("dp"), PAIR)
    block = term_ref.shape[0]
    steps = 2

    def sum_write(c):
        at = pl.ds(c * (block // steps), block // steps)
        return pltpu.make_async_copy(summed.at[at], dw_hbm.at[at], sems.at[1 + c])

    grad_write = pltpu.make_async_copy(grad_ref, grad_hbm, sems.at[0])
    grad_write.start()
    for c in range(steps):
        at = pl.ds(c * (block // steps), block // steps)
        up = jnp.where(z > 0, landed_ref[0, at, :].astype(jnp.float32), 0.0)
        down = jnp.where(z < LINE - 1, landed_ref[1, at, :].astype(jnp.float32), 0.0)
        summed[at, :] = (term_ref[at, :] + up + down) * factor
        sum_write(c).start()
    grad_write.wait()
    for c in range(steps):
        sum_write(c).wait()


def fused(out_grad, expert_of, pre_act, down_weight):
    experts = lax.axis_size("expert")
    replicas = lax.axis_size("dp")
    count, width = out_grad.shape
    rows, units = pre_act.shape
    block = down_weight.shape[1]
    capacity = count // 2
    factor = 1.0 / math.sqrt(replicas * count)
    half, full = jnp.bfloat16, jnp.float32
    hbm = pl.BlockSpec(memory_space=pltpu.HBM)
    anywhere = pl.BlockSpec(memory_space=pl.ANY)
    dma = pltpu.SemaphoreType.DMA
    placed = pl.pallas_call(
        functools.partial(kernel, experts, capacity),
        out_shape=(
            pltpu.VMEM((rows, units), half),
            pltpu.VMEM((block, width), full),
            pltpu.VMEM((2, block, width), half),
        ),
        in_specs=[hbm, hbm, hbm, hbm],
        out_specs=(anywhere, anywhere, anywhere),
        scratch_shapes=[
            pltpu.VMEM((count, width), half),
            pltpu.VMEM((1, count), jnp.int32),
            pltpu.VMEM((count, width), half),
            pltpu.VMEM((1, count), jnp.int32),
            pltpu.VMEM((2, experts * capacity, count), half),
            pltpu.VMEM((2, experts - 1, capacity, width), half),
            pltpu.VMEM((2, rows, width), half),
            pltpu.VMEM((LINE, rows, block), half),
            pltpu.VMEM((LINE, rows, block), half),
            pltpu.VMEM((2 * LANES, rows, block), half),
            pltpu.VMEM((2 * LANES, count, block), half),
            pltpu.VMEM((2 * LANES, count, block), half),
            pltpu.VMEM((2 * LANES, experts, capacity, block), half),
            pltpu.VMEM((LINE, block, width), half),
            pltpu.VMEM((2, LINE, rows, block), half),
            pltpu.VMEM((2, LINE, rows, block), full),
            pltpu.VMEM((LINE, block, width), full),
            pltpu.VMEM((LINE - 1, block, width), half),
            pltpu.VMEM((2, LINE - 2, block, width), half),
            dma((2,)),
            dma((3 + HALVES,)),
            dma((1,)),
            dma((HALVES,)),
            dma((LINE + 3 + LANES,)),
            dma((1 + (LINE - LANES) * CUTS,)),
            dma((2,)),
            dma((4, LANES)),
            dma((1 + 2 * LANES,)),
            dma((2,)),
            dma((LINE, PARTS)),
            dma((2,)),
            dma((2, CUTS * HALVES + CUTS + 1)),
            dma((3,)),
        ],
        compiler_params=pltpu.CompilerParams(
            collective_id=0, has_side_effects=True, vmem_limit_bytes=51 * 1024 * 1024
        ),
    )(*(
        pltpu.with_memory_space_constraint(array, pltpu.HBM)
        for array in (out_grad, expert_of.reshape(1, count), pre_act, down_weight[0])
    ))
    vmem = pl.BlockSpec(memory_space=pltpu.VMEM)
    pre_grad, summed = pl.pallas_call(
        functools.partial(finish, factor),
        out_shape=(
            jax.ShapeDtypeStruct((rows, units), half),
            jax.ShapeDtypeStruct((block, width), full),
        ),
        in_specs=[vmem, vmem, vmem],
        out_specs=(hbm, hbm),
        scratch_shapes=[pltpu.VMEM((block, width), full), dma((3,))],
        compiler_params=pltpu.CompilerParams(vmem_limit_bytes=16 * 1024 * 1024),
    )(*placed)
    return pre_grad, summed.reshape(1, block, width)


def body(out_grad, expert_of, pre_act, down_weight):
    experts = lax.axis_size("expert")
    replicas = lax.axis_size("dp")
    if replicas == PAIR * LINE and experts <= 8:
        return fused(out_grad, expert_of, pre_act, down_weight)
    token_count = out_grad.shape[0]
    model_width = out_grad.shape[1]
    capacity = token_count // 2
    routed = expert_of[:, 0]
    onehot = (routed[:, None] == jnp.arange(experts, dtype=jnp.int32)[None, :]).astype(jnp.int32)
    position = jnp.sum((jnp.cumsum(onehot, axis=0) - onehot) * onehot, axis=1)
    target = routed * capacity + position
    outgoing = jnp.zeros((experts * capacity, model_width), jnp.bfloat16).at[target].set(out_grad)
    arrived = lax.all_to_all(
        outgoing.reshape(experts, capacity, model_width),
        "expert",
        split_axis=0,
        concat_axis=0,
        tiled=True,
    )
    arrived = arrived.reshape(experts * capacity, model_width)
    weight = down_weight[0]
    own_rows = weight.shape[0]
    factor = 1.0 / math.sqrt(replicas * token_count)
    hidden_grad = lax.dot_general(
        arrived,
        lax.all_gather(weight, "dp", axis=0, tiled=True),
        (((1,), (1,)), ((), ())),
        preferred_element_type=jnp.float32,
    )
    pre_block = pre_act.astype(jnp.float32)
    pre_grad = (hidden_grad * derivative(pre_block)).astype(jnp.bfloat16)
    hidden = activate(pre_block).astype(jnp.bfloat16)
    summed = lax.psum_scatter(
        lax.dot_general(
            hidden, arrived, (((0,), (0,)), ((), ())), preferred_element_type=jnp.float32
        ),
        "dp",
        scatter_dimension=0,
        tiled=True,
    )
    return (pre_grad, (summed * factor).reshape(1, own_rows, model_width))


def solution(mesh):
    placed = (
        P(("dp", "expert"), None),
        P(("dp", "expert"), None),
        P(("dp", "expert"), None),
        P("expert", "dp", None),
    )
    return jax.shard_map(
        body,
        mesh=mesh,
        in_specs=placed,
        out_specs=(P(("dp", "expert"), None), P("expert", "dp", None)),
        check_vma=False,
    )
```

```python
import functools
import math

import jax
import jax.numpy as jnp
from jax import lax
from jax.experimental import pallas as pl
from jax.experimental.pallas import tpu as pltpu
from jax.sharding import PartitionSpec as P

tanh_scale = 0.7978845608028654
cubic_weight = 0.044715
MESH = pl.DeviceIdType.MESH
PAIR = 2
LINE = 4
CUTS = 2
HALVES = 2
PARTS = 2
LANES = 2


def activate(values):
    argument = tanh_scale * (values + cubic_weight * values * values * values)
    return 0.5 * values * (1.0 + jnp.tanh(argument))


def derivative(values):
    tangent = jnp.tanh(tanh_scale * (values + cubic_weight * values * values * values))
    return 0.5 * (1.0 + tangent) + 0.5 * values * (1.0 - tangent * tangent) * tanh_scale * (
        1.0 + 3.0 * cubic_weight * values * values
    )


def kernel(
    experts,
    capacity,
    tokens_hbm,
    route_hbm,
    pre_hbm,
    weight_hbm,
    grad_hbm,
    term_out,
    landed,
    own_tokens,
    own_route,
    their_tokens,
    their_route,
    choose,
    outgoing,
    arrived,
    pre_own,
    pre_theirs,
    lane_in,
    lane_pack,
    lane_got,
    lane_out,
    weights,
    hidden,
    slope,
    partial,
    sums_out,
    sums_in,
    input_sems,
    token_sems,
    dispatch_send,
    dispatch_recv,
    local_sems,
    pre_sems,
    lane_send,
    lane_recv,
    cross_sems,
    weight_send,
    weight_recv,
    sum_send,
    sum_recv,
    grad_sems,
):
    d = lax.axis_index("dp")
    me = lax.axis_index("expert")
    z = lax.div(d, PAIR)
    x = lax.rem(d, PAIR)
    partner = z * PAIR + 1 - x
    rows, width = pre_hbm.shape[0], own_tokens.shape[1]
    block = weight_hbm.shape[0]
    count = own_tokens.shape[0]
    low = z < LINE // 2
    own = LINE - 1
    direct = LINE - LANES
    piece, part_rows, span = block // CUTS, block // PARTS, width // HALVES

    def order(i):
        if i == own:
            return z
        down = LINE - 1 - i
        return jnp.where(
            low, jnp.where(down > z, down, down - 1), jnp.where(i < z, i, i + 1)
        )

    def columns(j, side):
        return pl.ds(pl.multiple_of((j * PAIR + side) * block, block), block)

    def within(cut):
        return pl.ds(cut * piece, piece)

    def across(half):
        return pl.ds(half * span, span)

    def slots(source):
        return pl.ds(pl.multiple_of(source * capacity, capacity), capacity)

    def peer(k):
        return lax.rem(me + k, experts)

    def from_peer(k):
        return lax.rem(me + experts - k, experts)

    route_load = pltpu.make_async_copy(route_hbm, own_route, input_sems.at[0])
    token_load = pltpu.make_async_copy(tokens_hbm, own_tokens, input_sems.at[1])
    weight_own = pltpu.make_async_copy(weight_hbm, weights.at[z], local_sems.at[1])
    weight_own.start()
    route_load.start()
    token_load.start()

    barrier = pltpu.get_barrier_semaphore()
    pl.semaphore_signal(barrier, inc=1, device_id={"dp": partner}, device_id_type=MESH)
    for k in range(1, experts):
        pl.semaphore_signal(
            barrier, inc=1, device_id={"expert": peer(k)}, device_id_type=MESH
        )

    @pl.when(z > 0)
    def _():
        pl.semaphore_signal(barrier, inc=1, device_id={"dp": d - PAIR}, device_id_type=MESH)

    @pl.when(z < LINE - 1)
    def _():
        pl.semaphore_signal(barrier, inc=1, device_id={"dp": d + PAIR}, device_id_type=MESH)

    inner = jnp.where((z > 0) & (z < LINE - 1), 2, 1)
    pl.semaphore_wait(barrier, experts + inner)

    def remote(src, dst, send, recv, device):
        return pltpu.make_async_remote_copy(
            src_ref=src, dst_ref=dst, send_sem=send, recv_sem=recv,
            device_id=device, device_id_type=MESH,
        )

    route_copy = remote(
        route_hbm, their_route, token_sems.at[0], token_sems.at[1],
        {"dp": partner},
    )

    def token_copy(half):
        return remote(
            own_tokens.at[:, across(half)], their_tokens.at[:, across(half)],
            token_sems.at[2], token_sems.at[3 + half], {"dp": partner},
        )

    def pre_copy(i, cut):
        start = (order(i) * PAIR + 1 - x) * block + cut * piece
        return remote(
            pre_hbm.at[:, pl.ds(pl.multiple_of(start, piece), piece)],
            pre_theirs.at[i, :, within(cut)],
            grad_sems.at[0], pre_sems.at[i * CUTS + cut], {"dp": partner},
        )

    def cross(lane):
        return remote(
            lane_pack.at[lane], lane_got.at[lane],
            cross_sems.at[0], cross_sems.at[1 + lane], {"dp": partner},
        )

    def part(c):
        return pl.ds(c * part_rows, part_rows)

    def weight_copy(direction, hop, c):
        step = 1 - 2 * direction
        shard = jnp.clip(z - step * hop, 0, LINE - 1)
        return remote(
            weights.at[shard, part(c)], weights.at[shard, part(c)], weight_send.at[direction],
            weight_recv.at[shard, c], {"dp": d + step * PAIR},
        )

    def sends(direction, hop):
        if direction == 0:
            return (z >= hop) & (z < LINE - 1)
        return (z <= LINE - 1 - hop) & (z > 0)

    def receives(direction, hop):
        return (z > hop) if direction == 0 else (z < LINE - 1 - hop)

    def weight_start(hop, c):
        for direction in range(2):
            @pl.when(sends(direction, hop))
            def _():
                weight_copy(direction, hop, c).start()

    def weight_arrive(hop, c):
        for direction in range(2):
            @pl.when(receives(direction, hop))
            def _():
                step = 1 - 2 * direction
                shard = jnp.clip(z - step * (hop + 1), 0, LINE - 1)
                remote(
                    weight_hbm.at[part(c)], weights.at[shard, part(c)],
                    weight_send.at[direction], weight_recv.at[shard, c], {"dp": partner},
                ).wait_recv()

        if hop < LINE - 2:
            weight_start(hop + 1, c)

    weight_own.wait()
    for c in range(PARTS):
        weight_start(0, c)
    route_copy.start()
    token_load.wait()
    for half in range(HALVES):
        token_copy(half).start()
    for i in range(direct):
        for cut in range(CUTS):
            pre_copy(i, cut).start()

    def own_copy(i):
        return pltpu.make_async_copy(
            pre_hbm.at[:, columns(order(i), x)], pre_own.at[i], local_sems.at[0]
        )

    for i in range(LINE):
        own_copy(i).start()
    earlier = (
        lax.broadcasted_iota(jnp.int32, (count, count), 0)
        < lax.broadcasted_iota(jnp.int32, (count, count), 1)
    ).astype(jnp.float32).astype(jnp.bfloat16)

    def plan(rep, routes):
        names = routes[...]
        named = lax.broadcasted_iota(jnp.int32, (8, count), 0) == names
        onehot = named.astype(jnp.float32)
        before = jnp.dot(
            onehot.astype(jnp.bfloat16), earlier, preferred_element_type=jnp.float32
        )
        position = jnp.sum(onehot * before, axis=0, keepdims=True).astype(jnp.int32)
        slot = lax.broadcasted_iota(jnp.int32, (capacity, count), 0)
        for e in range(experts):
            place = jnp.where(names == e, position, -1)
            choose[rep, e * capacity:(e + 1) * capacity, :] = (
                (slot == place).astype(jnp.float32).astype(jnp.bfloat16)
            )

    def dispatch_copy(rep, k, half):
        return remote(
            outgoing.at[rep, k - 1, :, across(half)],
            arrived.at[rep, slots(me), across(half)],
            dispatch_send.at[0],
            dispatch_recv.at[half],
            {"expert": peer(k)},
        )

    def dispatch(rep, tokens, half):
        for k in list(range(1, experts)) + [0]:
            rows_out = jnp.dot(
                choose[rep, slots(peer(k)), :], tokens[:, across(half)],
                preferred_element_type=jnp.float32,
            ).astype(jnp.bfloat16)
            if k == 0:
                arrived[rep, slots(me), across(half)] = rows_out
            else:
                outgoing[rep, k - 1, :, across(half)] = rows_out
                dispatch_copy(rep, k, half).start()

    peers = pl.ds(0, (experts - 1) * capacity)

    def tokens_arrive(half):
        came = arrived.at[:, peers, across(half)]
        remote(
            came, came, dispatch_send.at[0], dispatch_recv.at[half], {"expert": peer(1)}
        ).wait_recv()

    def lane_unit(lane):
        return own - lane

    def lane_columns(lane):
        return columns(order(lane_unit(lane)), 1 - x)

    def lane_target(leg, lane, source):
        if leg == 0:
            return lane_in.at[lane, slots(source)]
        if leg == 1:
            return pre_theirs.at[lane_unit(lane), slots(source)]
        if leg == 2:
            return lane_in.at[LANES + lane, slots(source)]
        return grad_hbm.at[slots(source), lane_columns(lane)]

    def lane_copy(leg, lane, k):
        if leg == 0:
            src = pre_hbm.at[slots(peer(k)), lane_columns(lane)]
        elif leg == 2:
            src = pre_theirs.at[lane_unit(lane), slots(peer(k))]
        else:
            src = lane_out.at[lane + LANES * (leg // 2), k]
        return remote(
            src, lane_target(leg, lane, me), lane_send.at[leg // 2], lane_recv.at[leg, lane],
            {"expert": peer(k)},
        )

    def lane_arrive(leg, lane):
        came = lane_in.at[lane, peers]
        remote(
            came, came, lane_send.at[0], lane_recv.at[leg, lane], {"expert": peer(1)}
        ).wait_recv()

    def lane_local(lane):
        return pltpu.make_async_copy(
            pre_hbm.at[slots(me), lane_columns(lane)], lane_in.at[lane, slots(me)],
            local_sems.at[4 + lane],
        )

    def lane_home(lane):
        return pltpu.make_async_copy(
            lane_out.at[LANES + lane, 0], grad_hbm.at[slots(me), lane_columns(lane)],
            local_sems.at[2],
        )

    def gather(way, lane):
        if way == 0:
            lane_local(lane).wait()
        lane_arrive(2 * way, lane)
        at = LANES * way + lane
        lane_pack[at] = lax.dot_general(
            choose[way], lane_in[at], (((0,), (0,)), ((), ())),
            preferred_element_type=jnp.float32,
        ).astype(jnp.bfloat16)
        cross(at).start()

    def spread(way, lane):
        at = LANES * way + lane
        cross(at).wait_recv()
        for k in list(range(1, experts)) + [0]:
            rows_out = jnp.dot(
                choose[1 - way, slots(peer(k)), :], lane_got[at],
                preferred_element_type=jnp.float32,
            ).astype(jnp.bfloat16)
            if way == 0 and k == 0:
                pre_theirs[lane_unit(lane), slots(me), :] = rows_out
            else:
                lane_out[at, k] = rows_out
                if k == 0:
                    lane_home(lane).start()
                else:
                    lane_copy(2 * way + 1, lane, k).start()

    strip = 64

    def activate_rows(rep, i, source, cut):
        at_columns = within(cut)

        @pl.loop(0, rows // (2 * strip))
        def _(t):
            for half in range(2):
                at = pl.ds(pl.multiple_of(t * 2 * strip + half * strip, strip), strip)
                v = source[i, at, at_columns].astype(jnp.float32)
                square = v * v
                tangent = jnp.tanh(tanh_scale * v * (1.0 + cubic_weight * square))
                gate = 0.5 * (1.0 + tangent)
                slope[rep, i, at, at_columns] = gate + 0.5 * v * (
                    1.0 - tangent * tangent
                ) * tanh_scale * (1.0 + 3.0 * cubic_weight * square)
                hidden[rep, i, at, at_columns] = (v * gate).astype(jnp.bfloat16)

    def activate_own(i):
        for cut in range(CUTS):
            activate_rows(0, i, pre_own, cut)

    def activate_theirs(i, cut):
        if i < direct:
            pre_copy(i, cut).wait_recv()
        activate_rows(1, i, pre_theirs, cut)

    def term(i, cut, half):
        at, wide = within(cut), across(half)
        total = lax.dot_general(
            hidden[0, i, :, at], arrived[0, :, wide], (((0,), (0,)), ((), ())),
            preferred_element_type=jnp.float32,
        )
        partial[i, at, wide] = total + lax.dot_general(
            hidden[1, i, :, at], arrived[1, :, wide], (((0,), (0,)), ((), ())),
            preferred_element_type=jnp.float32,
        )

    def terms(i):
        for cut in range(CUTS):
            for half in range(HALVES):
                term(i, cut, half)
            if i < own:
                begin(i, cut)

    def sum_copy(direction, stage, cut, half, i=0):
        at = within(cut)
        wide = pl.ds(0, width) if half is None else across(half)
        target = landed.at[direction] if stage == LINE - 2 else sums_in.at[direction, stage]
        slot = min(stage * CUTS + cut, 2 * CUTS)
        return remote(
            sums_out.at[i, at, wide], target.at[at, wide], sum_send.at[direction],
            sum_recv.at[direction, slot], {"dp": d + (1 - 2 * direction) * PAIR},
        )

    def toward(i, direction, ends):
        j = order(i)
        away = (j > z) if direction == 0 else (j < z)
        first = (z == 0) if direction == 0 else (z == LINE - 1)
        return away & first if ends else away & jnp.logical_not(first)

    def begin(i, cut, half=None):
        at = within(cut)
        wide = pl.ds(0, width) if half is None else across(half)
        for direction in range(2):
            @pl.when(toward(i, direction, True))
            def _():
                sums_out[i, at, wide] = partial[i, at, wide].astype(jnp.bfloat16)
                sum_copy(direction, i, cut, half, i).start()

    def forward(i, cut):
        at = within(cut)
        stage = min(i + 1, LINE - 2)
        for direction in range(2):
            @pl.when(toward(i, direction, False))
            def _():
                came = sums_in.at[direction, stage - 1, at]
                remote(
                    came, came, sum_send.at[direction],
                    sum_recv.at[direction, (stage - 1) * CUTS + cut], {"dp": partner},
                ).wait_recv()
                sums_out[i, at, :] = (
                    partial[i, at, :]
                    + sums_in[direction, stage - 1, at, :].astype(jnp.float32)
                ).astype(jnp.bfloat16)
                sum_copy(direction, stage, cut, None, i).start()

    def grad_copy(i):
        return remote(
            pre_theirs.at[i], grad_hbm.at[:, columns(order(i), x)],
            grad_sems.at[0], grad_sems.at[1], {"dp": partner},
        )

    def grad_write(i):
        return pltpu.make_async_copy(
            pre_own.at[i], grad_hbm.at[:, columns(order(i), x)], grad_sems.at[2]
        )

    tile = 256

    def differentiate(rep, i):
        j = order(i)
        result = pre_theirs if rep == 1 else pre_own

        @pl.loop(0, rows // tile)
        def _(t):
            at = pl.ds(pl.multiple_of(t * tile, tile), tile)
            product = lax.dot_general(
                arrived[rep, at, :], weights[j], (((1,), (1,)), ((), ())),
                preferred_element_type=jnp.float32,
            )
            result[i, at, :] = (product * slope[rep, i, at, :]).astype(jnp.bfloat16)

        if rep == 0:
            grad_write(i).start()
        elif i < direct:
            grad_copy(i).start()
        else:
            for k in range(1, experts):
                lane_copy(2, own - i, k).start()
            lane_in[LANES + own - i, slots(me), :] = pre_theirs[i, slots(me), :]

    route_load.wait()
    plan(0, own_route)
    dispatch(0, own_tokens, 0)
    pltpu.make_async_copy(pre_own, pre_own, local_sems.at[0]).wait()
    activate_own(0)
    activate_own(1)
    route_copy.wait_recv()
    plan(1, their_route)
    token_copy(0).wait_recv()
    dispatch(1, their_tokens, 0)
    dispatch(0, own_tokens, 1)
    activate_own(2)
    weight_arrive(0, 0)
    token_copy(1).wait_recv()
    dispatch(1, their_tokens, 1)
    for lane in range(LANES):
        lane_local(lane).start()
        for k in range(1, experts):
            lane_copy(0, lane, k).start()
    activate_own(own)
    tokens_arrive(0)
    for cut in range(CUTS):
        activate_theirs(0, cut)
        term(0, cut, 0)
        begin(0, cut, 0)
    weight_arrive(0, 1)
    tokens_arrive(1)
    for cut in range(CUTS):
        term(0, cut, 1)
        begin(0, cut, 1)
    differentiate(0, own)
    differentiate(0, own - 1)
    gather(0, 0)
    activate_theirs(1, 0)
    weight_arrive(1, 0)
    gather(0, 1)
    activate_theirs(1, 1)
    forward(0, 0)
    terms(1)
    spread(0, 0)
    forward(0, 1)
    weight_arrive(1, 1)
    spread(0, 1)
    differentiate(1, 1)
    differentiate(0, 1)
    lane_arrive(1, 0)
    for cut in range(CUTS):
        activate_theirs(own, cut)
    differentiate(1, own)
    terms(own)
    term_copy = pltpu.make_async_copy(
        partial.at[own], term_out, local_sems.at[3]
    )
    term_copy.start()
    lane_arrive(1, 1)
    for cut in range(CUTS):
        activate_theirs(own - 1, cut)
    terms(own - 1)
    differentiate(1, own - 1)
    forward(1, 0)
    forward(2, 0)
    weight_arrive(2, 0)
    gather(1, 0)
    gather(1, 1)
    forward(1, 1)
    forward(2, 1)
    weight_arrive(2, 1)
    differentiate(1, 0)
    differentiate(0, 0)
    for lane in range(LANES):
        spread(1, lane)

    for lane in range(LANES):
        lane_arrive(3, lane)
    home = lane_out.at[pl.ds(LANES, LANES), 0]
    pltpu.make_async_copy(home, home, local_sems.at[2]).wait()
    units = pre_theirs.at[pl.ds(0, direct)]
    returned = remote(units, units, grad_sems.at[0], grad_sems.at[1], {"dp": partner})
    returned.wait_recv()
    pltpu.make_async_copy(pre_own, pre_own, grad_sems.at[2]).wait()
    term_copy.wait()
    for direction in range(2):
        @pl.when(receives(direction, 0))
        def _():
            whole = landed.at[direction]
            remote(
                whole, whole, sum_send.at[direction],
                sum_recv.at[direction, 2 * CUTS], {"dp": partner},
            ).wait_recv()

    route_copy.wait_send()
    remote(
        own_tokens, their_tokens, token_sems.at[2], token_sems.at[3], {"dp": partner}
    ).wait_send()
    crossed = hidden.at[:, pl.ds(0, direct)]
    remote(
        crossed, crossed, grad_sems.at[0], grad_sems.at[1], {"dp": partner}
    ).wait_send()
    remote(
        lane_pack, lane_got, cross_sems.at[0], cross_sems.at[1], {"dp": partner}
    ).wait_send()
    remote(
        outgoing, outgoing, dispatch_send.at[0], dispatch_recv.at[0], {"expert": peer(1)}
    ).wait_send()
    lanes_sent = lane_in.at[:, peers]
    for way in range(2):
        remote(
            lanes_sent, lanes_sent, lane_send.at[way], lane_recv.at[0, 0], {"expert": peer(1)}
        ).wait_send()
    for n in range(1, LINE):
        for direction in range(2):
            @pl.when(z == (n - 1 if direction == 0 else LINE - n))
            def _():
                shards = weights.at[pl.ds(0, n)]
                remote(
                    shards, shards, weight_send.at[direction], weight_recv.at[0, 0],
                    {"dp": partner},
                ).wait_send()

            @pl.when(z == (LINE - 1 - n if direction == 0 else n))
            def _():
                sent = sums_out.at[pl.ds(0, n)]
                remote(
                    sent, sent, sum_send.at[direction], sum_recv.at[direction, 0],
                    {"dp": partner},
                ).wait_send()


def finish(factor, grad_ref, term_ref, landed_ref, grad_hbm, dw_hbm, summed, sems):
    z = lax.div(lax.axis_index("dp"), PAIR)
    block = term_ref.shape[0]
    steps = 2

    def sum_write(c):
        at = pl.ds(c * (block // steps), block // steps)
        return pltpu.make_async_copy(summed.at[at], dw_hbm.at[at], sems.at[1 + c])

    grad_write = pltpu.make_async_copy(grad_ref, grad_hbm, sems.at[0])
    grad_write.start()
    for c in range(steps):
        at = pl.ds(c * (block // steps), block // steps)
        up = jnp.where(z > 0, landed_ref[0, at, :].astype(jnp.float32), 0.0)
        down = jnp.where(z < LINE - 1, landed_ref[1, at, :].astype(jnp.float32), 0.0)
        summed[at, :] = (term_ref[at, :] + up + down) * factor
        sum_write(c).start()
    grad_write.wait()
    for c in range(steps):
        sum_write(c).wait()


def fused(out_grad, expert_of, pre_act, down_weight):
    experts = lax.axis_size("expert")
    replicas = lax.axis_size("dp")
    count, width = out_grad.shape
    rows, units = pre_act.shape
    block = down_weight.shape[1]
    capacity = count // 2
    factor = 1.0 / math.sqrt(replicas * count)
    half, full = jnp.bfloat16, jnp.float32
    hbm = pl.BlockSpec(memory_space=pltpu.HBM)
    anywhere = pl.BlockSpec(memory_space=pl.ANY)
    dma = pltpu.SemaphoreType.DMA
    placed = pl.pallas_call(
        functools.partial(kernel, experts, capacity),
        out_shape=(
            pltpu.VMEM((rows, units), half),
            pltpu.VMEM((block, width), full),
            pltpu.VMEM((2, block, width), half),
        ),
        in_specs=[hbm, hbm, hbm, hbm],
        out_specs=(anywhere, anywhere, anywhere),
        scratch_shapes=[
            pltpu.VMEM((count, width), half),
            pltpu.VMEM((1, count), jnp.int32),
            pltpu.VMEM((count, width), half),
            pltpu.VMEM((1, count), jnp.int32),
            pltpu.VMEM((2, experts * capacity, count), half),
            pltpu.VMEM((2, experts - 1, capacity, width), half),
            pltpu.VMEM((2, rows, width), half),
            pltpu.VMEM((LINE, rows, block), half),
            pltpu.VMEM((LINE, rows, block), half),
            pltpu.VMEM((2 * LANES, rows, block), half),
            pltpu.VMEM((2 * LANES, count, block), half),
            pltpu.VMEM((2 * LANES, count, block), half),
            pltpu.VMEM((2 * LANES, experts, capacity, block), half),
            pltpu.VMEM((LINE, block, width), half),
            pltpu.VMEM((2, LINE, rows, block), half),
            pltpu.VMEM((2, LINE, rows, block), full),
            pltpu.VMEM((LINE, block, width), full),
            pltpu.VMEM((LINE - 1, block, width), half),
            pltpu.VMEM((2, LINE - 2, block, width), half),
            dma((2,)),
            dma((3 + HALVES,)),
            dma((1,)),
            dma((HALVES,)),
            dma((4 + LANES,)),
            dma(((LINE - LANES) * CUTS,)),
            dma((2,)),
            dma((4, LANES)),
            dma((1 + 2 * LANES,)),
            dma((2,)),
            dma((LINE, PARTS)),
            dma((2,)),
            dma((2, 2 * CUTS + 1)),
            dma((3,)),
        ],
        compiler_params=pltpu.CompilerParams(
            collective_id=0, has_side_effects=True, vmem_limit_bytes=51 * 1024 * 1024
        ),
    )(*(
        pltpu.with_memory_space_constraint(array, pltpu.HBM)
        for array in (out_grad, expert_of.reshape(1, count), pre_act, down_weight[0])
    ))
    vmem = pl.BlockSpec(memory_space=pltpu.VMEM)
    pre_grad, summed = pl.pallas_call(
        functools.partial(finish, factor),
        out_shape=(
            jax.ShapeDtypeStruct((rows, units), half),
            jax.ShapeDtypeStruct((block, width), full),
        ),
        in_specs=[vmem, vmem, vmem],
        out_specs=(hbm, hbm),
        scratch_shapes=[pltpu.VMEM((block, width), full), dma((3,))],
        compiler_params=pltpu.CompilerParams(vmem_limit_bytes=16 * 1024 * 1024),
    )(*placed)
    return pre_grad, summed.reshape(1, block, width)


def body(out_grad, expert_of, pre_act, down_weight):
    experts = lax.axis_size("expert")
    replicas = lax.axis_size("dp")
    if replicas == PAIR * LINE and experts <= 8:
        return fused(out_grad, expert_of, pre_act, down_weight)
    token_count = out_grad.shape[0]
    model_width = out_grad.shape[1]
    capacity = token_count // 2
    routed = expert_of[:, 0]
    onehot = (routed[:, None] == jnp.arange(experts, dtype=jnp.int32)[None, :]).astype(jnp.int32)
    position = jnp.sum((jnp.cumsum(onehot, axis=0) - onehot) * onehot, axis=1)
    target = routed * capacity + position
    outgoing = jnp.zeros((experts * capacity, model_width), jnp.bfloat16).at[target].set(out_grad)
    arrived = lax.all_to_all(
        outgoing.reshape(experts, capacity, model_width),
        "expert",
        split_axis=0,
        concat_axis=0,
        tiled=True,
    )
    arrived = arrived.reshape(experts * capacity, model_width)
    weight = down_weight[0]
    own_rows = weight.shape[0]
    factor = 1.0 / math.sqrt(replicas * token_count)
    hidden_grad = lax.dot_general(
        arrived,
        lax.all_gather(weight, "dp", axis=0, tiled=True),
        (((1,), (1,)), ((), ())),
        preferred_element_type=jnp.float32,
    )
    pre_block = pre_act.astype(jnp.float32)
    pre_grad = (hidden_grad * derivative(pre_block)).astype(jnp.bfloat16)
    hidden = activate(pre_block).astype(jnp.bfloat16)
    summed = lax.psum_scatter(
        lax.dot_general(
            hidden, arrived, (((0,), (0,)), ((), ())), preferred_element_type=jnp.float32
        ),
        "dp",
        scatter_dimension=0,
        tiled=True,
    )
    return (pre_grad, (summed * factor).reshape(1, own_rows, model_width))


def solution(mesh):
    placed = (
        P(("dp", "expert"), None),
        P(("dp", "expert"), None),
        P(("dp", "expert"), None),
        P("expert", "dp", None),
    )
    return jax.shard_map(
        body,
        mesh=mesh,
        in_specs=placed,
        out_specs=(P(("dp", "expert"), None), P("expert", "dp", None)),
        check_vma=False,
    )
```
